256 devices in a mesh: own: 64 (over y, z, core), split: 4 (over x).
Axes of the slice: x: 4, y: 4, z: 8, core: 2. Of those that a mesh axis runs over, the one named last changes fastest.
Arguments:
- source_coords: float32 [256, 50, 256], P('own'), may hold values from -1.5 to 1.5
- target_coords: float32 [256, 50, 256], P('own'), may hold values from -1.5 to 1.5
- source_logmass: float32 [256, 256], P('own'), may hold values from -3 to 3
- target_logmass: float32 [256, 256], P('own'), may hold values from -3 to 3
- target_prior: float32 [256, 256], P('own'), may hold values from -6 to 121.5
- pair_source: int32 [64, 4, 64, 1], P('own', 'split'), may hold values from 0 to 3, as said below
- pair_target: int32 [64, 4, 64, 1], P('own', 'split'), may hold values from -1 to 3, as said below
Outputs:
- source_potential: float32 [256, 256], P('own')
- target_potential: float32 [256, 256], P('own')
The draws below stay inside these ranges and needn't reach their ends.
Inputs may be any that keep to these rules, and one draw needn't show every extreme that they name: `pair_source`: names one of the 4 source clusters of owner o. `pair_target`: -1 marks an empty slot. Live (source, target) pairs are all distinct; every source cluster and every target cluster is in some live pair. Bucket b of a device holds at most one pair whose target cluster belongs to owner b, and some device has all its slots live.
All inputs are finite; a program needn't handle non-finite values.
Results may differ from the reference program's by a relative error of at most 0.00011.
Values sent between devices are 32-bit elements; how exact they have to be, the bound alone decides.
No kernel may reach another device: no remote copies, remote signals or barrier semaphores. Data moves between devices by JAX's collectives and lax.ppermute only.
A program may use at most 128 MiB of HBM per device.

```python
import jax
import jax.numpy as jnp
from jax import lax

P_SIZE = 50
CELLS = 256
CL_DEV = 4
MOST = 1
CLUSTERS = 256
N_OWN = 64
N_SPLIT = 4


def pair_layout(key):
    base_key = jax.random.fold_in(key, 7)
    key_level, key_chosen, key_dice, key_shuffle, key_rotation = jax.random.split(base_key, 5)
    devices = N_OWN * N_SPLIT
    fill_level = jax.random.randint(key_level, (N_OWN, N_SPLIT), 1, 9)
    fill_level = jnp.maximum(fill_level * fill_level // 8, 1)
    chosen = jax.random.randint(key_chosen, (), 0, devices)
    device_rank = jnp.arange(devices, dtype=jnp.int32).reshape(N_OWN, N_SPLIT)
    fill_level = jnp.where(device_rank == chosen, 8, fill_level)
    dice_roll = jax.random.randint(key_dice, (N_OWN, N_SPLIT, N_OWN, MOST), 0, 8)
    living = dice_roll < fill_level[:, :, None, None]
    combo_count = CL_DEV * CL_DEV
    shuffle_keys = jax.random.randint(key_shuffle, (N_OWN, N_OWN, combo_count), 0, 2 ** 20)
    shuffle_keys = shuffle_keys * combo_count + jnp.arange(combo_count, dtype=jnp.int32)
    shuffle = jnp.argsort(shuffle_keys, axis=-1).astype(jnp.int32)
    picked_combos = shuffle[:, :, :N_SPLIT * MOST].reshape(N_OWN, N_OWN, N_SPLIT, MOST)
    picked_combos = jnp.transpose(picked_combos, (0, 2, 1, 3))
    source_pick = picked_combos // CL_DEV
    target_pick = picked_combos % CL_DEV
    slot_rank = (jnp.arange(N_SPLIT, dtype=jnp.int32)[:, None] * MOST + jnp.arange(MOST, dtype=jnp.int32)[None, :])[None, :, None, :]
    rotation = jax.random.randint(key_rotation, (N_OWN, 1, 1, 1), 0, CL_DEV)
    diagonal_source = slot_rank % CL_DEV
    diagonal_target = (diagonal_source + slot_rank // CL_DEV + rotation) % CL_DEV
    own_bucket = jnp.arange(N_OWN, dtype=jnp.int32)[:, None, None, None] == jnp.arange(N_OWN, dtype=jnp.int32)[None, None, :, None]
    source_pick = jnp.where(own_bucket, diagonal_source, source_pick)
    target_pick = jnp.where(own_bucket, diagonal_target, target_pick)
    living = living | own_bucket
    target_pick = jnp.where(living, target_pick, -1)
    return (source_pick.astype(jnp.int32), target_pick.astype(jnp.int32))


def draw_pair_source(key, part):
    return pair_layout(key)[0]


def draw_pair_target(key, part):
    return pair_layout(key)[1]


def draw_target_prior(key, part):
    key_normal = jax.random.fold_in(jax.random.fold_in(key, 11), 0)
    return jnp.clip(jax.random.normal(key_normal, (CLUSTERS, CELLS), jnp.float32), -6.0, 6.0)


def shard_levels(key, dims, cuts, smallest, largest):
    loudness = 1.0
    for dim, shards_of in cuts:
        draws = jax.random.uniform(jax.random.fold_in(jax.random.fold_in(key, 6), dim), (shards_of,), jnp.float32, smallest / len(cuts), largest / len(cuts))
        loudness = loudness * jnp.repeat(jnp.exp(draws), dims[dim] // shards_of).reshape((-1,) + (1,) * (len(dims) - 1 - dim))
    return loudness


def centred(own_key, extent, width, bound, shards=(), kind=jnp.bfloat16):
    drawn = jax.random.normal(own_key, extent, jnp.float32) * width
    if len(shards) > 0:
        drawn = shard_levels(own_key, extent, shards, -0.22, 0.18) * drawn
    return jnp.clip(drawn, min=-bound, max=bound).astype(kind)


def setup_inputs(seed: int = 0) -> dict:
    keys = jax.random.split(jax.random.key(seed), 8)
    return {
        "source_coords": centred(keys[0], (CLUSTERS, P_SIZE, CELLS), 0.25, 1.5, ((0, 64),), jnp.float32),
        "target_coords": centred(keys[1], (CLUSTERS, P_SIZE, CELLS), 0.25, 1.5, ((0, 64),), jnp.float32),
        "source_logmass": centred(keys[2], (CLUSTERS, CELLS), 0.5, 3.0, ((0, 64),), jnp.float32),
        "target_logmass": centred(keys[3], (CLUSTERS, CELLS), 0.5, 3.0, ((0, 64),), jnp.float32),
        "target_prior": draw_target_prior(jax.random.fold_in(keys[7], 71), 0),
        "pair_source": draw_pair_source(jax.random.fold_in(keys[7], 71), 0),
        "pair_target": draw_pair_target(jax.random.fold_in(keys[7], 71), 0),
    }


EPSILON = 0.5
NEGATIVE = -1.0e30


def pair_costs(left_part, right_part):
    inner_sum = jnp.einsum("bpi,bpj->bij", left_part, right_part, precision=lax.Precision.HIGHEST)
    source_norm = jnp.sum(left_part * left_part, axis=1)
    target_norm = jnp.sum(right_part * right_part, axis=1)
    return source_norm[:, :, None] + target_norm[:, None, :] - 2.0 * inner_sum


def reference(source_coords, target_coords, source_logmass, target_logmass, target_prior, pair_source, pair_target):
    owner_ids = jnp.arange(N_OWN, dtype=jnp.int32)[:, None, None, None]
    bucket_ids = jnp.arange(N_OWN, dtype=jnp.int32)[None, None, :, None]
    source_ids = (owner_ids * CL_DEV + pair_source).reshape(-1, 64).astype(jnp.int32)
    target_ids = (bucket_ids * CL_DEV + jnp.maximum(pair_target, 0)).reshape(-1, 64).astype(jnp.int32)
    living = (pair_target >= 0).reshape(-1, 64)
    start_ceiling = jnp.full((CLUSTERS, CELLS), NEGATIVE, jnp.float32)
    start_amount = jnp.zeros((CLUSTERS, CELLS), jnp.float32)

    def row_round(running, lists):
        ceiling, amount = running
        anchor, target, alive_rows = lists
        pair_cost = pair_costs(source_coords[anchor], target_coords[target])
        exponent = (target_prior[target][:, None, :] - pair_cost) / EPSILON
        summit = jnp.max(exponent, axis=2)
        weights = jnp.sum(jnp.exp(exponent - summit[:, :, None]), axis=2)
        summit = jnp.where(alive_rows[:, None], summit, NEGATIVE)
        weights = jnp.where(alive_rows[:, None], weights, 0.0)
        new_ceiling = ceiling.at[anchor].max(summit)
        added = jnp.zeros_like(amount).at[anchor].add(weights * jnp.exp(summit - new_ceiling[anchor]))
        return (new_ceiling, amount * jnp.exp(ceiling - new_ceiling) + added), None

    (row_ceiling, row_amount), _ = lax.scan(row_round, (start_ceiling, start_amount), (source_ids, target_ids, living))
    source_potential = EPSILON * source_logmass - EPSILON * (row_ceiling + jnp.log(row_amount))

    def column_round(running, lists):
        ceiling, amount = running
        anchor, target, alive_rows = lists
        pair_cost = pair_costs(source_coords[anchor], target_coords[target])
        exponent = (source_potential[anchor][:, :, None] - pair_cost) / EPSILON
        summit = jnp.max(exponent, axis=1)
        weights = jnp.sum(jnp.exp(exponent - summit[:, None, :]), axis=1)
        summit = jnp.where(alive_rows[:, None], summit, NEGATIVE)
        weights = jnp.where(alive_rows[:, None], weights, 0.0)
        new_ceiling = ceiling.at[target].max(summit)
        added = jnp.zeros_like(amount).at[target].add(weights * jnp.exp(summit - new_ceiling[target]))
        return (new_ceiling, amount * jnp.exp(ceiling - new_ceiling) + added), None

    (col_ceiling, col_amount), _ = lax.scan(column_round, (start_ceiling, start_amount), (source_ids, target_ids, living))
    target_potential = EPSILON * target_logmass - EPSILON * (col_ceiling + jnp.log(col_amount))
    return source_potential, target_potential
```

```python
import math

import jax
import jax.numpy as jnp
from jax import lax
from jax.experimental import pallas as pl
from jax.experimental.pallas import tpu as pltpu
from jax.sharding import PartitionSpec as P

EPSILON = 0.5
NEGATIVE = -1e30
LN2 = math.log(2.0)
SCALE = 1.0 / (EPSILON * LN2)

COMP = 50
CL = 4
CELLS = 256
NY, NZ, NC, NX = 4, 8, 2, 4
AXES = ("own", "split")

Z_FIRST = (0, 1, 2, 3)
Z_SECOND = (4, -1, -2, -3)

BLOCK = 64
PRODUCTS = ((0, 0), (0, 1), (1, 0), (1, 1), (0, 2), (2, 0))
DEPTH = BLOCK * len(PRODUCTS)
SLOTS = 64
GROUP = 2
LIST = SLOTS + 8

f32, bf16 = jnp.float32, jnp.bfloat16


def device(x, y, z, c):
    return (((y % NY) * NZ + z % NZ) * NC + c % NC) * NX + x % NX


def fetched(value, source):
    pairs = [
        (device(*source(x, y, z, c)), device(x, y, z, c))
        for y in range(NY)
        for z in range(NZ)
        for c in range(NC)
        for x in range(NX)
    ]
    return lax.ppermute(value, AXES, pairs)


def from_x(value, k):
    return fetched(value, lambda x, y, z, c: (x + k, y, z, c))


def from_y(value, k):
    return fetched(value, lambda x, y, z, c: (x, y + k, z, c))


def from_core(value):
    return fetched(value, lambda x, y, z, c: (x, y, z, c + 1))


def three_parts(v):
    high = v.astype(bf16).astype(f32)
    rest = v - high
    middle = rest.astype(bf16).astype(f32)
    return high, middle, rest - middle


def load_cluster(ref, a):
    top = ref[a, 0:48, :]
    tail = ref[a, 48:56, :]
    row = lax.broadcasted_iota(jnp.int32, (8, CELLS), 0)
    extra = tail[2:3, :]
    tail = jnp.where(row < 2, tail, 0.0)
    square = jnp.sum(top * top, axis=0, keepdims=True) + jnp.sum(tail * tail, axis=0, keepdims=True)
    return top, tail, extra, square


def with_rows(tail, first, second):
    row = lax.broadcasted_iota(jnp.int32, (8, CELLS), 0)
    for k in range(3):
        tail = jnp.where(row == 2 + k, first[k], tail)
        tail = jnp.where(row == 5 + k, second[k], tail)
    return tail


def store_operand(put, top, tail, side, first, second):
    tops, tails = three_parts(top), three_parts(tail)
    zeros = jnp.zeros((8, CELLS), f32)
    for n, product in enumerate(PRODUCTS):
        part = product[side]
        end = with_rows(tails[part], first, second) if n == 0 else tails[part]
        put(n * BLOCK, tops[part].astype(bf16))
        put(n * BLOCK + 48, jnp.concatenate([end, zeros], axis=0).astype(bf16))


def logsum(top, total):
    return jnp.where(total > 0.0, top + jnp.log2(total), NEGATIVE)


def merged(parts):
    top = parts[0]
    for part in parts[1:]:
        top = jnp.maximum(top, part)
    total = sum(jnp.exp2(part - top) for part in parts)
    return top + jnp.log2(total)


def over_pairs(count, list_ref, left_ref, right_ref, pick, top_ref, sum_ref):
    def step(q, carry):
        for r in range(GROUP):
            pair = list_ref[q * GROUP + r]
            source, target = pair >> 8, pair & 255
            left, right, place = pick(source, target)
            e = jnp.dot(left_ref[left], right_ref[right], preferred_element_type=f32)
            e = e.reshape(CELLS // 8, 8, CELLS)
            old = top_ref[place]
            new = jnp.maximum(old, jnp.max(e, axis=0))
            total = jnp.sum(jnp.exp2(e - new[None]), axis=0)
            sum_ref[place] = sum_ref[place] * jnp.exp2(old - new) + total
            top_ref[place] = new
        return carry

    lax.fori_loop(0, (count + GROUP - 1) // GROUP, step, 0)


def finish(top_ref, sum_ref):
    tops, sums = top_ref[0 : 4 * CL], sum_ref[0 : 4 * CL]
    top = jnp.max(tops, axis=1, keepdims=True)
    total = jnp.sum(sums * jnp.exp2(tops - top), axis=1)
    return logsum(top[:, 0, :], total)


def row_kernel(codes, owners, s0, s1, s2, s3, t0, t1, t2, t3, out, list_ref, xn, yn, yt, top, tot):
    one = jnp.ones((1, CELLS), f32)
    ones = (one, one, one)
    for k, ref in enumerate((s0, s1, s2, s3)):
        for a in range(CL):
            head, tail, _, square = load_cluster(ref, a)

            def put(at, v, n=k * CL + a):
                xn[n, at : at + v.shape[0], :] = v

            weight = three_parts(-square * SCALE)
            store_operand(put, head * (2.0 * SCALE), tail * (2.0 * SCALE), 0, weight, ones)
    xn[4 * CL] = jnp.zeros((DEPTH, CELLS), bf16)
    for k, ref in enumerate((t0, t1, t2, t3)):
        for a in range(CL):
            head, tail, prior, square = load_cluster(ref, a)

            def put(at, v):
                yn[at : at + v.shape[0], :] = v

            weight = three_parts((prior - square) * SCALE)
            store_operand(put, head, tail, 1, ones, weight)
            yt[k * CL + a] = yn[...].T
    count = jnp.int32(0)
    for k in range(4):
        for d in range(NX):
            for t in range(4):
                code = codes[k * NX + d, owners[t]]
                source = k * CL + (code >> 2)
                list_ref[count] = source * 256 + t * CL + (code & 3)
                count = count + (code >= 0).astype(jnp.int32)
    for k in range(GROUP):
        list_ref[count + k] = 4 * CL * 256
    list_ref[LIST - 1] = count
    top[...] = jnp.full(top.shape, NEGATIVE, f32)
    tot[...] = jnp.zeros(tot.shape, f32)
    over_pairs(count, list_ref, yt, xn, lambda s, t: (t, s, s), top, tot)
    out[...] = finish(top, tot)


def column_kernel(list_ref, m0, m1, m2, m3, s0, s1, s2, s3, t0, t1, t2, t3, out, potential, xn, xt, yn, top, tot):
    one = jnp.ones((1, CELLS), f32)
    ones = (one, one, one)
    came = (m0, m1, m2, m3)
    for k, ref in enumerate((s0, s1, s2, s3)):
        for a in range(CL):
            head, tail, mass, square = load_cluster(ref, a)
            rows = [came[d][((k - d) % 4) * CL + a : ((k - d) % 4) * CL + a + 1, :] for d in range(4)]
            p = EPSILON * mass - (EPSILON * LN2) * merged(rows)
            if k == 0:
                potential[a : a + 1, :] = p

            def put(at, v):
                xn[at : at + v.shape[0], :] = v

            weight = three_parts((p - square) * SCALE)
            store_operand(put, head * (2.0 * SCALE), tail * (2.0 * SCALE), 0, weight, ones)
            xt[k * CL + a] = xn[...].T
    for k, ref in enumerate((t0, t1, t2, t3)):
        for a in range(CL):
            head, tail, _, square = load_cluster(ref, a)

            def put(at, v, n=k * CL + a):
                yn[n, at : at + v.shape[0], :] = v

            weight = three_parts(-square * SCALE)
            store_operand(put, head, tail, 1, ones, weight)
    xt[4 * CL] = jnp.zeros((CELLS, DEPTH), bf16)
    top[...] = jnp.full(top.shape, NEGATIVE, f32)
    tot[...] = jnp.zeros(tot.shape, f32)

    def pick(s, t):
        return s, t, jnp.where(s == 4 * CL, 4 * CL, t)

    over_pairs(list_ref[LIST - 1], list_ref, xt, yn, pick, top, tot)
    out[...] = finish(top, tot)


VMEM = pl.BlockSpec(memory_space=pltpu.VMEM)
SMEM = pl.BlockSpec(memory_space=pltpu.SMEM)


def body(source_coords, target_coords, source_logmass, target_logmass, target_prior, pair_source, pair_target):
    x = lax.axis_index("split")
    own = lax.axis_index("own")
    y, z, c = own // (NZ * NC), (own // NC) % NZ, own % NC
    shifts = jnp.array((Z_FIRST, Z_SECOND), jnp.int32)[:, x]
    near = y * (NZ * NC) + ((z + shifts) % NZ) * NC
    owners = jnp.stack([near + c, near + (1 - c)], axis=1).reshape(4).astype(jnp.int32)

    codes = pair_source * 4 + pair_target
    codes = jnp.where(pair_target >= 0, codes, -1).reshape(1, -1)
    codes = jnp.concatenate([codes] + [from_x(codes, k) for k in (1, 2, 3)], axis=0)
    codes = jnp.concatenate([codes] + [from_y(codes, k) for k in (1, 2, 3)], axis=0)

    def packed(coords, extra):
        zeros = jnp.zeros((CL, 5, CELLS), f32)
        return jnp.concatenate([coords, extra[:, None, :], zeros], axis=1)

    s0 = packed(source_coords, source_logmass)
    t = packed(target_coords, target_prior)
    t0 = fetched(t, lambda x, y, z, c: (x, y, z + Z_FIRST[x], c))
    t2 = fetched(t, lambda x, y, z, c: (x, y, z + Z_SECOND[x], c))
    s1, s2, s3 = (from_y(s0, k) for k in (1, 2, 3))
    t1, t3 = from_core(t0), from_core(t2)
    shards = (s0, s1, s2, s3, t0, t1, t2, t3)

    accumulators = [pltpu.VMEM((4 * CL + 1, 8, CELLS), f32)] * 2
    params = pltpu.CompilerParams(vmem_limit_bytes=56 * 2**20)
    rows, pairs = pl.pallas_call(
        row_kernel,
        out_shape=(
            jax.ShapeDtypeStruct((4 * CL, CELLS), f32),
            jax.ShapeDtypeStruct((LIST,), jnp.int32),
        ),
        in_specs=[SMEM, SMEM] + [VMEM] * 8,
        out_specs=(VMEM, SMEM),
        scratch_shapes=[
            pltpu.VMEM((4 * CL + 1, DEPTH, CELLS), bf16),
            pltpu.VMEM((DEPTH, CELLS), bf16),
            pltpu.VMEM((4 * CL, CELLS, DEPTH), bf16),
        ]
        + accumulators,
        compiler_params=params,
        name="rows",
    )(codes, owners, *shards)

    rows = merged([rows] + [from_x(rows, k) for k in (1, 2, 3)])
    others = [from_y(rows, k) for k in (1, 2, 3)]

    columns, source_potential = pl.pallas_call(
        column_kernel,
        out_shape=(
            jax.ShapeDtypeStruct((4 * CL, CELLS), f32),
            jax.ShapeDtypeStruct((CL, CELLS), f32),
        ),
        in_specs=[SMEM] + [VMEM] * 12,
        out_specs=(VMEM, VMEM),
        scratch_shapes=[
            pltpu.VMEM((DEPTH, CELLS), bf16),
            pltpu.VMEM((4 * CL + 1, CELLS, DEPTH), bf16),
            pltpu.VMEM((4 * CL, DEPTH, CELLS), bf16),
        ]
        + accumulators,
        compiler_params=params,
        name="columns",
    )(pairs, rows, *others, *shards)

    columns = columns.reshape(2, 2, CL, CELLS)
    kept = merged([columns[:, 0], from_core(columns[:, 1])])
    first = fetched(kept[0], lambda x, y, z, c: (x, y, z - Z_FIRST[x], c))
    second = fetched(kept[1], lambda x, y, z, c: (x, y, z - Z_SECOND[x], c))
    part = merged([first, second])
    part = merged([part] + [from_x(part, k) for k in (1, 2, 3)])
    target_potential = EPSILON * target_logmass - (EPSILON * LN2) * part
    return source_potential, target_potential


def solution(mesh):
    return jax.shard_map(
        body,
        mesh=mesh,
        in_specs=(
            P("own", None, None),
            P("own", None, None),
            P("own", None),
            P("own", None),
            P("own", None),
            P("own", "split", None, None),
            P("own", "split", None, None),
        ),
        out_specs=(P("own", None), P("own", None)),
        check_vma=False,
    )
```

```python
import math

import jax
import jax.numpy as jnp
from jax import lax
from jax.experimental import pallas as pl
from jax.experimental.pallas import tpu as pltpu
from jax.sharding import PartitionSpec as P


EPSILON = 0.5
NEGATIVE = -1e30
LN2 = math.log(2.0)
SCALE = 1.0 / (EPSILON * LN2)

CL = 4
CELLS = 256
NY, NZ, NC, NX = 4, 8, 2, 4
AXES = ("own", "split")

FAR = NZ // 2

BLOCK = 64
PRODUCTS = ((0, 0), (0, 1), (1, 0), (1, 1))
DEPTH = BLOCK * len(PRODUCTS)
SLOTS = 64
LIST = SLOTS + 8

f32, bf16 = jnp.float32, jnp.bfloat16


def device(x, y, z, c):
    return (((y % NY) * NZ + z % NZ) * NC + c % NC) * NX + x % NX


def fetched(value, source):
    pairs = [
        (device(*source(x, y, z, c)), device(x, y, z, c))
        for y in range(NY)
        for z in range(NZ)
        for c in range(NC)
        for x in range(NX)
    ]
    return lax.ppermute(value, AXES, pairs)


def from_x(value, k):
    return fetched(value, lambda x, y, z, c: (x + k, y, z, c))


def from_y(value, k):
    return fetched(value, lambda x, y, z, c: (x, y + k, z, c))


def from_core(value):
    return fetched(value, lambda x, y, z, c: (x, y, z, c + 1))


def three_parts(v):
    high = v.astype(bf16).astype(f32)
    rest = v - high
    middle = rest.astype(bf16).astype(f32)
    return high, middle, rest - middle


def target_owners():
    own, x = lax.axis_index("own"), lax.axis_index("split")
    row, z, c = (own // (NZ * NC)) * (NZ * NC), (own // NC) % NZ, own % NC
    near = row + ((z + x) % NZ) * NC
    far = row + ((z + x + NZ // 2) % NZ) * NC
    return near + c, near + 1 - c, far + c, far + 1 - c


def centre(ref):
    middle = jnp.mean(ref[0], axis=1, keepdims=True)
    return jnp.broadcast_to(middle, (56, CELLS))


def load_cluster(ref, a, middle):
    top = ref[a, 0:48, :] - middle[0:48]
    tail = ref[a, 48:56, :]
    row = lax.broadcasted_iota(jnp.int32, (8, CELLS), 0)
    extra = tail[2:3, :]
    tail = jnp.where(row < 2, tail - middle[48:56], 0.0)
    square = jnp.sum(top * top, axis=0, keepdims=True) + jnp.sum(tail * tail, axis=0, keepdims=True)
    return top, tail, extra, square


def with_rows(tail, first, second):
    row = lax.broadcasted_iota(jnp.int32, (8, CELLS), 0)
    for k in range(3):
        tail = jnp.where(row == 2 + k, first[k], tail)
        tail = jnp.where(row == 5 + k, second[k], tail)
    return tail


def store_operand(put, top, tail, side, first, second):
    tops, tails = three_parts(top), three_parts(tail)
    zeros = jnp.zeros((8, CELLS), f32)
    for n, product in enumerate(PRODUCTS):
        part = product[side]
        end = with_rows(tails[part], first, second) if n == 0 else tails[part]
        put(n * BLOCK, tops[part].astype(bf16))
        put(n * BLOCK + 48, jnp.concatenate([end, zeros], axis=0).astype(bf16))


def logsum(top, total):
    return jnp.where(total > 0.0, top + jnp.log2(total), NEGATIVE)


def merged(parts):
    top = parts[0]
    for part in parts[1:]:
        top = jnp.maximum(top, part)
    total = sum(jnp.exp2(part - top) for part in parts)
    return top + jnp.log2(total)


def over_pairs(count, list_ref, left_ref, right_ref, pick, top_ref, sum_ref, even, odd):
    def multiply(n, e_ref):
        pair = list_ref[n]
        left, right, _ = pick(pair >> 8, pair & 255)
        e_ref[...] = jnp.dot(left_ref[left], right_ref[right], preferred_element_type=f32)

    def absorb(n, e_ref):
        pair = list_ref[n]
        _, _, place = pick(pair >> 8, pair & 255)
        e = e_ref[...].reshape(CELLS // 8, 8, CELLS)
        top = jnp.max(e, axis=0)
        total = jnp.sum(jnp.exp2(e - top[None]), axis=0)
        old = top_ref[place]
        new = jnp.maximum(old, top)
        sum_ref[place] = sum_ref[place] * jnp.exp2(old - new) + total * jnp.exp2(top - new)
        top_ref[place] = new

    def step(q, carry):
        multiply(2 * q + 1, odd)
        absorb(2 * q, even)
        multiply(2 * q + 2, even)
        absorb(2 * q + 1, odd)
        return carry

    multiply(0, even)
    lax.fori_loop(0, (count + 1) // 2, step, 0)


def finish(top_ref, sum_ref):
    tops, sums = top_ref[0 : 4 * CL], sum_ref[0 : 4 * CL]
    top = jnp.max(tops, axis=1, keepdims=True)
    total = jnp.sum(sums * jnp.exp2(tops - top), axis=1)
    return logsum(top[:, 0, :], total)


def row_kernel(c0, c1, c2, c3, s0, s1, s2, s3, t0, t1, t2, t3, out, list_ref, xn, yn, yt, top, tot, even, odd):
    one = jnp.ones((1, CELLS), f32)
    ones = (one, one, one)
    middle = centre(s0)
    for k, ref in enumerate((s0, s1, s2, s3)):
        for a in range(CL):
            head, tail, _, square = load_cluster(ref, a, middle)

            def put(at, v, n=k * CL + a):
                xn[n, at : at + v.shape[0], :] = v

            weight = three_parts(-square * SCALE)
            store_operand(put, head * (2.0 * SCALE), tail * (2.0 * SCALE), 0, weight, ones)
    xn[4 * CL] = jnp.zeros((DEPTH, CELLS), bf16)
    for k, ref in enumerate((t0, t1, t2, t3)):
        for a in range(CL):
            head, tail, prior, square = load_cluster(ref, a, middle)

            def put(at, v):
                yn[at : at + v.shape[0], :] = v

            weight = three_parts((prior - square) * SCALE)
            store_operand(put, head, tail, 1, ones, weight)
            yt[k * CL + a] = yn[...].T
    owners = target_owners()
    count = jnp.int32(0)
    for k, codes in enumerate((c0, c1, c2, c3)):
        for d in range(NX):
            for t in range(4):
                code = codes[d, owners[t]]
                source = k * CL + (code >> 2)
                list_ref[count] = source * 256 + t * CL + (code & 3)
                count = count + (code >= 0).astype(jnp.int32)
    for k in range(2):
        list_ref[count + k] = 4 * CL * 256
    list_ref[LIST - 1] = count
    top[...] = jnp.full(top.shape, NEGATIVE, f32)
    tot[...] = jnp.zeros(tot.shape, f32)
    over_pairs(count, list_ref, yt, xn, lambda s, t: (t, s, s), top, tot, even, odd)
    out[...] = finish(top, tot)


def column_kernel(list_ref, m0, m1, m2, m3, s0, s1, s2, s3, t0, t1, t2, t3, kept, given, potential, xn, xt, yn, top, tot, even, odd):
    one = jnp.ones((1, CELLS), f32)
    ones = (one, one, one)
    middle = centre(s0)
    came = (m0, m1, m2, m3)
    for k, ref in enumerate((s0, s1, s2, s3)):
        for a in range(CL):
            head, tail, mass, square = load_cluster(ref, a, middle)
            rows = [came[d][((k - d) % 4) * CL + a : ((k - d) % 4) * CL + a + 1, :] for d in range(4)]
            p = EPSILON * mass - (EPSILON * LN2) * merged(rows)
            if k == 0:
                potential[a : a + 1, :] = p

            def put(at, v):
                xn[at : at + v.shape[0], :] = v

            weight = three_parts((p - square) * SCALE)
            store_operand(put, head * (2.0 * SCALE), tail * (2.0 * SCALE), 0, weight, ones)
            xt[k * CL + a] = xn[...].T
    for k, ref in enumerate((t0, t1, t2, t3)):
        for a in range(CL):
            head, tail, _, square = load_cluster(ref, a, middle)

            def put(at, v, n=k * CL + a):
                yn[n, at : at + v.shape[0], :] = v

            weight = three_parts(-square * SCALE)
            store_operand(put, head, tail, 1, ones, weight)
    xt[4 * CL] = jnp.zeros((CELLS, DEPTH), bf16)
    top[...] = jnp.full(top.shape, NEGATIVE, f32)
    tot[...] = jnp.zeros(tot.shape, f32)

    def pick(s, t):
        return s, t, jnp.where(s == 4 * CL, 4 * CL, t)

    over_pairs(list_ref[LIST - 1], list_ref, xt, yn, pick, top, tot, even, odd)
    columns = finish(top, tot)
    for k in range(2):
        kept[k * CL : (k + 1) * CL, :] = columns[2 * k * CL : (2 * k + 1) * CL]
        given[k * CL : (k + 1) * CL, :] = columns[(2 * k + 1) * CL : (2 * k + 2) * CL]


VMEM = pl.BlockSpec(memory_space=pltpu.VMEM)
SMEM = pl.BlockSpec(memory_space=pltpu.SMEM)


def work(source_coords, target_coords, source_logmass, target_logmass, target_prior, pair_source, pair_target):
    codes = pair_source * 4 + pair_target
    codes = jnp.where(pair_target >= 0, codes, -1).reshape(1, -1)
    codes = jnp.concatenate([codes] + [from_x(codes, k) for k in (1, 2, 3)], axis=0)
    codes = (codes,) + tuple(from_y(codes, k) for k in (1, 2, 3))

    def packed(coords, extra):
        zeros = jnp.zeros((CL, 5, CELLS), f32)
        return jnp.concatenate([coords, extra[:, None, :], zeros], axis=1)

    s0 = packed(source_coords, source_logmass)
    t = packed(target_coords, target_prior)
    t2 = fetched(t, lambda x, y, z, c: (x, y, z + x + FAR, c))
    t0 = fetched(t, lambda x, y, z, c: (x, y, z + x, c))
    s1, s2, s3 = (from_y(s0, k) for k in (1, 2, 3))
    t1, t3 = from_core(t0), from_core(t2)
    shards = (s0, s1, s2, s3, t0, t1, t2, t3)

    accumulators = [pltpu.VMEM((4 * CL + 1, 8, CELLS), f32)] * 2 + [pltpu.VMEM((CELLS, CELLS), f32)] * 2
    params = pltpu.CompilerParams(vmem_limit_bytes=16 * 2**20)
    rows, pairs = pl.pallas_call(
        row_kernel,
        out_shape=(
            jax.ShapeDtypeStruct((4 * CL, CELLS), f32),
            jax.ShapeDtypeStruct((LIST,), jnp.int32),
        ),
        in_specs=[SMEM] * 4 + [VMEM] * 8,
        out_specs=(VMEM, SMEM),
        scratch_shapes=[
            pltpu.VMEM((4 * CL + 1, DEPTH, CELLS), bf16),
            pltpu.VMEM((DEPTH, CELLS), bf16),
            pltpu.VMEM((4 * CL, CELLS, DEPTH), bf16),
        ]
        + accumulators,
        compiler_params=params,
        name="rows",
    )(*codes, *shards)

    rows = merged([rows] + [from_x(rows, k) for k in (1, 2, 3)])
    others = [from_y(rows, k) for k in (1, 2, 3)]

    kept, given, source_potential = pl.pallas_call(
        column_kernel,
        out_shape=(
            jax.ShapeDtypeStruct((2 * CL, CELLS), f32),
            jax.ShapeDtypeStruct((2 * CL, CELLS), f32),
            jax.ShapeDtypeStruct((CL, CELLS), f32),
        ),
        in_specs=[SMEM] + [VMEM] * 12,
        out_specs=(VMEM, VMEM, VMEM),
        scratch_shapes=[
            pltpu.VMEM((DEPTH, CELLS), bf16),
            pltpu.VMEM((4 * CL + 1, CELLS, DEPTH), bf16),
            pltpu.VMEM((4 * CL, DEPTH, CELLS), bf16),
        ]
        + accumulators,
        compiler_params=params,
        name="columns",
    )(pairs, rows, *others, *shards)

    kept = merged([kept, from_core(given)])
    first = fetched(kept[:CL], lambda x, y, z, c: (x, y, z - x, c))
    second = fetched(kept[CL:], lambda x, y, z, c: (x, y, z - x - FAR, c))
    part = merged([first, second])
    part = merged([part] + [from_x(part, k) for k in (1, 2, 3)])
    target_potential = EPSILON * target_logmass - (EPSILON * LN2) * part
    return source_potential, target_potential


def solution(mesh):
    return jax.shard_map(
        work,
        mesh=mesh,
        in_specs=(
            P("own", None, None),
            P("own", None, None),
            P("own", None),
            P("own", None),
            P("own", None),
            P("own", "split", None, None),
            P("own", "split", None, None),
        ),
        out_specs=(P("own", None), P("own", None)),
        check_vma=False,
    )
```

```python
import math

import jax
import jax.numpy as jnp
from jax import lax
from jax.experimental import pallas as pl
from jax.experimental.pallas import tpu as pltpu
from jax.sharding import PartitionSpec as P


EPSILON = 0.5
NEGATIVE = -1e30
LN2 = math.log(2.0)
SCALE = 1.0 / (EPSILON * LN2)

CL = 4
CELLS = 256
NY, NZ, NC, NX = 4, 8, 2, 4
AXES = ("own", "split")

FAR = NZ // 2

BLOCK = 64
PRODUCTS = ((0, 0), (0, 1), (1, 0), (1, 1))
DEPTH = BLOCK * len(PRODUCTS)
SLOTS = 64
LIST = SLOTS + 8

f32, bf16 = jnp.float32, jnp.bfloat16


def device(x, y, z, c):
    return (((y % NY) * NZ + z % NZ) * NC + c % NC) * NX + x % NX


def fetched(value, source):
    pairs = [
        (device(*source(x, y, z, c)), device(x, y, z, c))
        for y in range(NY)
        for z in range(NZ)
        for c in range(NC)
        for x in range(NX)
    ]
    return lax.ppermute(value, AXES, pairs)


def from_y(value, k):
    return fetched(value, lambda x, y, z, c: (x, y + k, z, c))


PLANES = [[device(x, y, z, c) for x in range(NX) for y in range(NY)] for z in range(NZ) for c in range(NC)]
SHARERS = [
    [device(x, y, z - x + FAR * e, c) for x in range(NX) for e in range(2) for c in range(NC)]
    for y in range(NY)
    for z in range(FAR)
]
MEMBERS = 16


def exchanged(value, groups):
    return lax.all_to_all(value, AXES, 0, 0, axis_index_groups=groups, tiled=True)


def from_core(value):
    return fetched(value, lambda x, y, z, c: (x, y, z, c + 1))


def three_parts(v):
    high = v.astype(bf16).astype(f32)
    rest = v - high
    middle = rest.astype(bf16).astype(f32)
    return high, middle, rest - middle


def place():
    own, x = lax.axis_index("own"), lax.axis_index("split")
    return x, own // (NZ * NC), (own // NC) % NZ, own % NC


def target_owners():
    x, y, z, c = place()
    row = y * (NZ * NC)
    near = row + ((z + x) % NZ) * NC
    far = row + ((z + x + NZ // 2) % NZ) * NC
    return near + c, near + 1 - c, far + c, far + 1 - c


def centre(ref):
    middle = jnp.mean(ref[0], axis=1, keepdims=True)
    return jnp.broadcast_to(middle, (56, CELLS))


def load_cluster(ref, a, middle):
    top = ref[a, 0:48, :] - middle[0:48]
    tail = ref[a, 48:56, :]
    row = lax.broadcasted_iota(jnp.int32, (8, CELLS), 0)
    extra = tail[2:3, :]
    tail = jnp.where(row < 2, tail - middle[48:56], 0.0)
    square = jnp.sum(top * top, axis=0, keepdims=True) + jnp.sum(tail * tail, axis=0, keepdims=True)
    return top, tail, extra, square


def with_rows(tail, first, second):
    row = lax.broadcasted_iota(jnp.int32, (8, CELLS), 0)
    for k in range(3):
        tail = jnp.where(row == 2 + k, first[k], tail)
        tail = jnp.where(row == 5 + k, second[k], tail)
    return tail


def store_operand(put, top, tail, side, first, second):
    tops, tails = three_parts(top), three_parts(tail)
    zeros = jnp.zeros((8, CELLS), f32)
    for n, product in enumerate(PRODUCTS):
        part = product[side]
        end = with_rows(tails[part], first, second) if n == 0 else tails[part]
        put(n * BLOCK, tops[part].astype(bf16))
        put(n * BLOCK + 48, jnp.concatenate([end, zeros], axis=0).astype(bf16))


def logsum(top, total):
    return jnp.where(total > 0.0, top + jnp.log2(total), NEGATIVE)


def merged(parts):
    top = parts[0]
    for part in parts[1:]:
        top = jnp.maximum(top, part)
    total = sum(jnp.exp2(part - top) for part in parts)
    return top + jnp.log2(total)


def over_pairs(count, list_ref, left_ref, right_ref, pick, top_ref, sum_ref, even, odd):
    def multiply(n, e_ref):
        pair = list_ref[n]
        left, right, _ = pick(pair >> 8, pair & 255)
        e_ref[...] = jnp.dot(left_ref[left], right_ref[right], preferred_element_type=f32)

    def absorb(n, e_ref):
        pair = list_ref[n]
        _, _, place = pick(pair >> 8, pair & 255)
        e = e_ref[...].reshape(CELLS // 8, 8, CELLS)
        top = jnp.max(e, axis=0)
        total = jnp.sum(jnp.exp2(e - top[None]), axis=0)
        old = top_ref[place]
        new = jnp.maximum(old, top)
        sum_ref[place] = sum_ref[place] * jnp.exp2(old - new) + total * jnp.exp2(top - new)
        top_ref[place] = new

    def step(q, carry):
        multiply(2 * q + 1, odd)
        absorb(2 * q, even)
        multiply(2 * q + 2, even)
        absorb(2 * q + 1, odd)
        return carry

    multiply(0, even)
    lax.fori_loop(0, (count + 1) // 2, step, 0)


def finish(top_ref, sum_ref):
    tops, sums = top_ref[0 : 4 * CL], sum_ref[0 : 4 * CL]
    top = jnp.max(tops, axis=1, keepdims=True)
    total = jnp.sum(sums * jnp.exp2(tops - top), axis=1)
    return logsum(top[:, 0, :], total)


def row_kernel(codes, s0, s1, s2, s3, t0, t1, t2, t3, out, list_ref, xn, yn, yt, top, tot, even, odd):
    one = jnp.ones((1, CELLS), f32)
    ones = (one, one, one)
    middle = centre(s0)
    for k, ref in enumerate((s0, s1, s2, s3)):
        for a in range(CL):
            head, tail, _, square = load_cluster(ref, a, middle)

            def put(at, v, n=k * CL + a):
                xn[n, at : at + v.shape[0], :] = v

            weight = three_parts(-square * SCALE)
            store_operand(put, head * (2.0 * SCALE), tail * (2.0 * SCALE), 0, weight, ones)
    xn[4 * CL] = jnp.zeros((DEPTH, CELLS), bf16)
    for k, ref in enumerate((t0, t1, t2, t3)):
        for a in range(CL):
            head, tail, prior, square = load_cluster(ref, a, middle)

            def put(at, v):
                yn[at : at + v.shape[0], :] = v

            weight = three_parts((prior - square) * SCALE)
            store_operand(put, head, tail, 1, ones, weight)
            yt[k * CL + a] = yn[...].T
    owners = target_owners()
    count = jnp.int32(0)
    y = place()[1]
    for k in range(4):
        for d in range(NX):
            for t in range(4):
                code = codes[d * NY + (y + k) % NY, owners[t]]
                source = k * CL + (code >> 2)
                list_ref[count] = source * 256 + t * CL + (code & 3)
                count = count + (code >= 0).astype(jnp.int32)
    for k in range(2):
        list_ref[count + k] = 4 * CL * 256
    list_ref[LIST - 1] = count
    top[...] = jnp.full(top.shape, NEGATIVE, f32)
    tot[...] = jnp.zeros(tot.shape, f32)
    over_pairs(count, list_ref, yt, xn, lambda s, t: (t, s, s), top, tot, even, odd)
    rows = finish(top, tot).reshape(4, CL, CELLS)
    for k in range(4):
        for m in range(MEMBERS):
            out[m, (y + k) % NY] = rows[k]


def column_kernel(list_ref, came, s0, s1, s2, s3, t0, t1, t2, t3, out, potential, xn, xt, yn, top, tot, even, odd, four):
    one = jnp.ones((1, CELLS), f32)
    ones = (one, one, one)
    middle = centre(s0)
    x, y, z, c = place()
    four[...] = merged([came[m] for m in range(MEMBERS)])
    for k, ref in enumerate((s0, s1, s2, s3)):
        rows = four[(y + k) % NY]
        for a in range(CL):
            head, tail, mass, square = load_cluster(ref, a, middle)
            p = EPSILON * mass - (EPSILON * LN2) * rows[a : a + 1]
            if k == 0:
                potential[a : a + 1, :] = p

            def put(at, v):
                xn[at : at + v.shape[0], :] = v

            weight = three_parts((p - square) * SCALE)
            store_operand(put, head * (2.0 * SCALE), tail * (2.0 * SCALE), 0, weight, ones)
            xt[k * CL + a] = xn[...].T
    for k, ref in enumerate((t0, t1, t2, t3)):
        for a in range(CL):
            head, tail, _, square = load_cluster(ref, a, middle)

            def put(at, v, n=k * CL + a):
                yn[n, at : at + v.shape[0], :] = v

            weight = three_parts(-square * SCALE)
            store_operand(put, head, tail, 1, ones, weight)
    xt[4 * CL] = jnp.zeros((CELLS, DEPTH), bf16)
    top[...] = jnp.full(top.shape, NEGATIVE, f32)
    tot[...] = jnp.zeros(tot.shape, f32)

    def pick(s, t):
        return s, t, jnp.where(s == 4 * CL, 4 * CL, t)

    over_pairs(list_ref[LIST - 1], list_ref, xt, yn, pick, top, tot, even, odd)
    four[...] = finish(top, tot).reshape(4, CL, CELLS)
    half = ((z + x) // FAR) % 2
    for f in range(2):
        for core in range(NC):
            part = four[2 * (f ^ half) + (core ^ c)]
            for d in range(NX):
                out[(d * 2 + f) * NC + core] = part


VMEM = pl.BlockSpec(memory_space=pltpu.VMEM)
SMEM = pl.BlockSpec(memory_space=pltpu.SMEM)


def work(source_coords, target_coords, source_logmass, target_logmass, target_prior, pair_source, pair_target):
    codes = pair_source * 4 + pair_target
    codes = jnp.where(pair_target >= 0, codes, -1).reshape(1, -1)
    codes = exchanged(jnp.broadcast_to(codes, (MEMBERS, codes.shape[1])), PLANES)

    def packed(coords, extra):
        zeros = jnp.zeros((CL, 5, CELLS), f32)
        return jnp.concatenate([coords, extra[:, None, :], zeros], axis=1)

    s0 = packed(source_coords, source_logmass)
    t = packed(target_coords, target_prior)
    t2 = fetched(t, lambda x, y, z, c: (x, y, z + x + FAR, c))
    t0 = fetched(t, lambda x, y, z, c: (x, y, z + x, c))
    s1, s2, s3 = (from_y(s0, k) for k in (1, 2, 3))
    t1, t3 = from_core(t0), from_core(t2)
    shards = (s0, s1, s2, s3, t0, t1, t2, t3)

    accumulators = [pltpu.VMEM((4 * CL + 1, 8, CELLS), f32)] * 2 + [pltpu.VMEM((CELLS, CELLS), f32)] * 2
    params = pltpu.CompilerParams(vmem_limit_bytes=16 * 2**20)
    rows, pairs = pl.pallas_call(
        row_kernel,
        out_shape=(
            jax.ShapeDtypeStruct((MEMBERS, 4, CL, CELLS), f32),
            jax.ShapeDtypeStruct((LIST,), jnp.int32),
        ),
        in_specs=[SMEM] + [VMEM] * 8,
        out_specs=(VMEM, SMEM),
        scratch_shapes=[
            pltpu.VMEM((4 * CL + 1, DEPTH, CELLS), bf16),
            pltpu.VMEM((DEPTH, CELLS), bf16),
            pltpu.VMEM((4 * CL, CELLS, DEPTH), bf16),
        ]
        + accumulators,
        compiler_params=params,
        name="rows",
    )(codes, *shards)

    rows = exchanged(rows, PLANES)

    columns, source_potential = pl.pallas_call(
        column_kernel,
        out_shape=(
            jax.ShapeDtypeStruct((MEMBERS, CL, CELLS), f32),
            jax.ShapeDtypeStruct((CL, CELLS), f32),
        ),
        in_specs=[SMEM] + [VMEM] * 9,
        out_specs=(VMEM, VMEM),
        scratch_shapes=[
            pltpu.VMEM((DEPTH, CELLS), bf16),
            pltpu.VMEM((4 * CL + 1, CELLS, DEPTH), bf16),
            pltpu.VMEM((4 * CL, DEPTH, CELLS), bf16),
        ]
        + accumulators
        + [pltpu.VMEM((4, CL, CELLS), f32)],
        compiler_params=params,
        name="columns",
    )(pairs, rows, *shards)

    part = merged(list(exchanged(columns, SHARERS)))
    part = fetched(part, lambda x, y, z, c: (x, y, z - x, c))
    target_potential = EPSILON * target_logmass - (EPSILON * LN2) * part
    return source_potential, target_potential


def solution(mesh):
    return jax.shard_map(
        work,
        mesh=mesh,
        in_specs=(
            P("own", None, None),
            P("own", None, None),
            P("own", None),
            P("own", None),
            P("own", None),
            P("own", "split", None, None),
            P("own", "split", None, None),
        ),
        out_specs=(P("own", None), P("own", None)),
        check_vma=False,
    )
```

```python
import math

import jax
import jax.numpy as jnp
from jax import lax
from jax.experimental import pallas as pl
from jax.experimental.pallas import tpu as pltpu
from jax.sharding import PartitionSpec as P


EPSILON = 0.5
NEGATIVE = -1e30
LN2 = math.log(2.0)
SCALE = 1.0 / (EPSILON * LN2)

CL = 4
CELLS = 256
NY, NZ, NC, NX = 4, 8, 2, 4
AXES = ("own", "split")

FAR = NZ // 2

BLOCK = 64
DEPTH = 2 * BLOCK
SLOTS = 64
DEEP = 4
LIST = SLOTS + 16

f32, bf16 = jnp.float32, jnp.bfloat16


def device(x, y, z, c):
    return (((y % NY) * NZ + z % NZ) * NC + c % NC) * NX + x % NX


def fetched(value, source):
    pairs = [
        (device(*source(x, y, z, c)), device(x, y, z, c))
        for y in range(NY)
        for z in range(NZ)
        for c in range(NC)
        for x in range(NX)
    ]
    return lax.ppermute(value, AXES, pairs)


def from_x(value, k):
    return fetched(value, lambda x, y, z, c: (x + k, y, z, c))


def from_y(value, k):
    return fetched(value, lambda x, y, z, c: (x, y + k, z, c))


PLANES = [[device(x, y, z, c) for x in range(NX) for y in range(NY)] for z in range(NZ) for c in range(NC)]
MEMBERS = 16


def exchanged(value, groups):
    return lax.all_to_all(value, AXES, 0, 0, axis_index_groups=groups, tiled=True)


def from_core(value):
    return fetched(value, lambda x, y, z, c: (x, y, z, c + 1))


def three_parts(v):
    high = v.astype(bf16).astype(f32)
    rest = v - high
    middle = rest.astype(bf16).astype(f32)
    return high, middle, rest - middle


def place():
    own, x = lax.axis_index("own"), lax.axis_index("split")
    return x, own // (NZ * NC), (own // NC) % NZ, own % NC


def target_owners():
    x, y, z, c = place()
    row = y * (NZ * NC)
    near = row + ((z + x) % NZ) * NC
    far = row + ((z + x + NZ // 2) % NZ) * NC
    return near + c, near + 1 - c, far + c, far + 1 - c


def centre(ref):
    middle = jnp.mean(ref[0], axis=1, keepdims=True)
    return jnp.broadcast_to(middle, (56, CELLS))


def load_cluster(ref, a, middle):
    top = ref[a, 0:48, :] - middle[0:48]
    tail = ref[a, 48:56, :]
    row = lax.broadcasted_iota(jnp.int32, (8, CELLS), 0)
    extra = tail[2:3, :]
    tail = jnp.where(row < 2, tail - middle[48:56], 0.0)
    square = jnp.sum(top * top, axis=0, keepdims=True) + jnp.sum(tail * tail, axis=0, keepdims=True)
    return top, tail, extra, square


def with_rows(tail, first, second):
    row = lax.broadcasted_iota(jnp.int32, (8, CELLS), 0)
    for k in range(3):
        tail = jnp.where(row == 2 + k, first[k], tail)
        tail = jnp.where(row == 5 + k, second[k], tail)
    return tail


def store_operand(ref, n, top, tail, first, second):
    zeros = jnp.zeros((8, CELLS), f32)
    for part, (head, end) in enumerate(zip(three_parts(top)[:2], three_parts(tail)[:2])):
        end = with_rows(end, first, second) if part == 0 else end
        at = part * BLOCK
        ref[n, at : at + 48, :] = head.astype(bf16)
        ref[n, at + 48 : at + BLOCK, :] = jnp.concatenate([end, zeros], axis=0).astype(bf16)


def logsum(top, total):
    return jnp.where(total > 0.0, top + jnp.log2(total), NEGATIVE)


def merged(parts):
    top = parts[0]
    for part in parts[1:]:
        top = jnp.maximum(top, part)
    total = sum(jnp.exp2(part - top) for part in parts)
    return top + jnp.log2(total)


def over_pairs(count, list_ref, left_ref, right_ref, pick, top_ref, sum_ref, scores, tops):
    def multiply(n, k):
        pair = list_ref[n]
        left, right, _ = pick(pair >> 8, pair & 255)
        cells = left_ref[left]
        high, low = right_ref[right, 0:BLOCK, :], right_ref[right, BLOCK:DEPTH, :]
        e = jnp.dot(
            jnp.concatenate([cells, cells], axis=1),
            jnp.concatenate([high, high, low, low], axis=0),
            preferred_element_type=f32,
        )
        scores[k][...] = e
        tops[k][...] = jnp.max(e.reshape(CELLS // 8, 8, CELLS), axis=0)

    def absorb(n, k):
        pair = list_ref[n]
        _, _, place = pick(pair >> 8, pair & 255)
        top = tops[k][...]
        e = scores[k][...].reshape(CELLS // 8, 8, CELLS)
        total = jnp.sum(jnp.exp2(e - top[None]), axis=0)
        old = top_ref[place]
        new = jnp.maximum(old, top)
        sum_ref[place] = sum_ref[place] * jnp.exp2(old - new) + total * jnp.exp2(top - new)
        top_ref[place] = new

    def step(q, carry):
        absorb(4 * q + 0, 0)
        multiply(4 * q + 4, 0)
        absorb(4 * q + 1, 1)
        multiply(4 * q + 5, 1)
        absorb(4 * q + 2, 2)
        multiply(4 * q + 6, 2)
        absorb(4 * q + 3, 3)
        multiply(4 * q + 7, 3)
        return carry

    multiply(0, 0)
    multiply(1, 1)
    multiply(2, 2)
    multiply(3, 3)
    lax.fori_loop(0, (count + 3) // 4, step, 0)


def finish(top_ref, sum_ref):
    tops, sums = top_ref[0 : 4 * CL], sum_ref[0 : 4 * CL]
    top = jnp.max(tops, axis=1, keepdims=True)
    total = jnp.sum(sums * jnp.exp2(tops - top), axis=1)
    return logsum(top[:, 0, :], total)


def row_kernel(codes_in, s0, s1, s2, s3, t0, t1, t2, t3, out, list_out, xn, yn, mass, square_out, codes, list_ref, yt, top, tot, *rest):
    scores, tops, sem = rest[:DEEP], rest[DEEP : 2 * DEEP], rest[2 * DEEP]
    arriving = pltpu.make_async_copy(codes_in, codes, sem.at[0])
    arriving.start()
    one = jnp.ones((1, CELLS), f32)
    ones = (one, one, one)
    middle = centre(s0)
    for k, ref in enumerate((s0, s1, s2, s3)):
        for a in range(CL):
            head, tail, extra, square = load_cluster(ref, a, middle)
            mass[k * CL + a : k * CL + a + 1, :] = extra
            square_out[k * CL + a : k * CL + a + 1, :] = square
            weight = three_parts(-square * SCALE)
            store_operand(xn, k * CL + a, head * (2.0 * SCALE), tail * (2.0 * SCALE), weight, ones)
    top[...] = jnp.full(top.shape, NEGATIVE, f32)
    tot[...] = jnp.zeros(tot.shape, f32)
    arriving.wait()
    owners = target_owners()
    count = jnp.int32(0)
    y = place()[1]
    for k in range(4):
        for d in range(NX):
            for t in range(4):
                code = codes[d * NY + (y + k) % NY, owners[t]]
                source = k * CL + (code >> 2)
                list_ref[count] = source * 256 + t * CL + (code & 3)
                count = count + (code >= 0).astype(jnp.int32)
    for k in range(2 * DEEP):
        list_ref[count + k] = 4 * CL * 256
    list_ref[LIST - 1] = count
    leaving = pltpu.make_async_copy(list_ref, list_out, sem.at[1])
    leaving.start()
    xn[4 * CL] = jnp.zeros((DEPTH, CELLS), bf16)
    for k, ref in enumerate((t0, t1, t2, t3)):
        for a in range(CL):
            head, tail, prior, square = load_cluster(ref, a, middle)
            weight = three_parts((prior - square) * SCALE)
            store_operand(yn, k * CL + a, head, tail, ones, weight)
            yt[k * CL + a] = yn[k * CL + a].T
    over_pairs(count, list_ref, yt, xn, lambda s, t: (t, s, s), top, tot, scores, tops)
    rows = finish(top, tot).reshape(4, CL, CELLS)
    for k in range(4):
        for m in range(MEMBERS):
            out[m, (y + k) % NY] = rows[k]
    leaving.wait()


def column_kernel(list_in, came, mass, square, x_in, yn, kept, given, potential, list_ref, xn, xt, four, top, tot, *rest):
    scores, tops, sem = rest[:DEEP], rest[DEEP : 2 * DEEP], rest[2 * DEEP]
    arriving = pltpu.make_async_copy(list_in, list_ref, sem.at[0])
    arriving.start()
    y = place()[1]
    four[...] = merged([came[m] for m in range(MEMBERS)])
    row = lax.broadcasted_iota(jnp.int32, (16, CELLS), 0)
    for k in range(4):
        rows = four[(y + k) % NY]
        for a in range(CL):
            n = k * CL + a
            p = EPSILON * mass[n : n + 1, :] - (EPSILON * LN2) * rows[a : a + 1]
            if k == 0:
                potential[a : a + 1, :] = p
            weight = three_parts((p - square[n : n + 1, :]) * SCALE)
            xn[...] = x_in[n]
            end = xn[48:64, :].astype(f32)
            for part in range(3):
                end = jnp.where(row == 2 + part, weight[part], end)
            xn[48:64, :] = end.astype(bf16)
            xt[n] = xn[...].T
    xt[4 * CL] = jnp.zeros((CELLS, DEPTH), bf16)
    top[...] = jnp.full(top.shape, NEGATIVE, f32)
    tot[...] = jnp.zeros(tot.shape, f32)
    arriving.wait()

    def pick(s, t):
        return s, t, jnp.where(s == 4 * CL, 4 * CL, t)

    over_pairs(list_ref[LIST - 1], list_ref, xt, yn, pick, top, tot, scores, tops)
    columns = finish(top, tot)
    for k in range(2):
        kept[k * CL : (k + 1) * CL, :] = columns[2 * k * CL : (2 * k + 1) * CL]
        given[k * CL : (k + 1) * CL, :] = columns[(2 * k + 1) * CL : (2 * k + 2) * CL]


VMEM = pl.BlockSpec(memory_space=pltpu.VMEM)
ANY = pl.BlockSpec(memory_space=pl.ANY)


def work(source_coords, target_coords, source_logmass, target_logmass, target_prior, pair_source, pair_target):
    codes = pair_source * 4 + pair_target
    codes = jnp.where(pair_target >= 0, codes, -1).reshape(1, -1)
    codes = exchanged(jnp.broadcast_to(codes, (MEMBERS, codes.shape[1])), PLANES)

    def packed(coords, extra):
        zeros = jnp.zeros((CL, 5, CELLS), f32)
        return jnp.concatenate([coords, extra[:, None, :], zeros], axis=1)

    s0 = packed(source_coords, source_logmass)
    t = packed(target_coords, target_prior)
    t2 = fetched(t, lambda x, y, z, c: (x, y, z + x + FAR, c))
    t0 = fetched(t, lambda x, y, z, c: (x, y, z + x, c))
    s1, s2, s3 = (from_y(s0, k) for k in (1, 2, 3))
    t1, t3 = from_core(t0), from_core(t2)
    shards = (s0, s1, s2, s3, t0, t1, t2, t3)

    shared = (
        [pltpu.VMEM((4 * CL + 1, 8, CELLS), f32)] * 2
        + [pltpu.VMEM((CELLS, CELLS), f32)] * DEEP
        + [pltpu.VMEM((8, CELLS), f32)] * DEEP
        + [pltpu.SemaphoreType.DMA((2,))]
    )
    params = pltpu.CompilerParams(vmem_limit_bytes=16 * 2**20)
    rows, pairs, xn, yn, mass, square = pl.pallas_call(
        row_kernel,
        out_shape=(
            jax.ShapeDtypeStruct((MEMBERS, 4, CL, CELLS), f32),
            jax.ShapeDtypeStruct((LIST,), jnp.int32),
            jax.ShapeDtypeStruct((4 * CL + 1, DEPTH, CELLS), bf16),
            jax.ShapeDtypeStruct((4 * CL, DEPTH, CELLS), bf16),
            jax.ShapeDtypeStruct((4 * CL, CELLS), f32),
            jax.ShapeDtypeStruct((4 * CL, CELLS), f32),
        ),
        in_specs=[ANY] + [VMEM] * 8,
        out_specs=(VMEM, ANY, VMEM, VMEM, VMEM, VMEM),
        scratch_shapes=[
            pltpu.SMEM((MEMBERS, SLOTS), jnp.int32),
            pltpu.SMEM((LIST,), jnp.int32),
            pltpu.VMEM((4 * CL, CELLS, DEPTH), bf16),
        ]
        + shared,
        compiler_params=params,
        name="rows",
    )(codes, *shards)

    rows = exchanged(rows, PLANES)

    kept, given, source_potential = pl.pallas_call(
        column_kernel,
        out_shape=(
            jax.ShapeDtypeStruct((2 * CL, CELLS), f32),
            jax.ShapeDtypeStruct((2 * CL, CELLS), f32),
            jax.ShapeDtypeStruct((CL, CELLS), f32),
        ),
        in_specs=[ANY] + [VMEM] * 5,
        out_specs=(VMEM, VMEM, VMEM),
        scratch_shapes=[
            pltpu.SMEM((LIST,), jnp.int32),
            pltpu.VMEM((DEPTH, CELLS), bf16),
            pltpu.VMEM((4 * CL + 1, CELLS, DEPTH), bf16),
            pltpu.VMEM((4, CL, CELLS), f32),
        ]
        + shared,
        compiler_params=params,
        name="columns",
    )(pairs, rows, mass, square, xn, yn)

    kept = merged([kept, from_core(given)])
    first = fetched(kept[:CL], lambda x, y, z, c: (x, y, z - x, c))
    second = fetched(kept[CL:], lambda x, y, z, c: (x, y, z - x - FAR, c))
    part = merged([first, second])
    part = merged([part] + [from_x(part, k) for k in (1, 2, 3)])
    target_potential = EPSILON * target_logmass + target_prior - (EPSILON * LN2) * part
    return source_potential, target_potential


def solution(mesh):
    return jax.shard_map(
        work,
        mesh=mesh,
        in_specs=(
            P("own", None, None),
            P("own", None, None),
            P("own", None),
            P("own", None),
            P("own", None),
            P("own", "split", None, None),
            P("own", "split", None, None),
        ),
        out_specs=(P("own", None), P("own", None)),
        check_vma=False,
    )
```

```python
import math

import jax
import jax.numpy as jnp
from jax import lax
from jax.experimental import pallas as pl
from jax.experimental.pallas import tpu as pltpu
from jax.sharding import PartitionSpec as P


EPSILON = 0.5
NEGATIVE = -1e30
LN2 = math.log(2.0)
SCALE = 1.0 / (EPSILON * LN2)

COMP = 50
CL = 4
CELLS = 256
PACKED = 56
NY, NZ, NC, NX = 4, 8, 2, 4
AXES = ("own", "split")

FAR = NZ // 2

BLOCK = 64
DEPTH = 2 * BLOCK
SLOTS = 64
DEEP = 4
LIST = SLOTS + 16

f32, bf16 = jnp.float32, jnp.bfloat16


def device(x, y, z, c):
    return (((y % NY) * NZ + z % NZ) * NC + c % NC) * NX + x % NX


def fetched(value, source):
    pairs = [
        (device(*source(x, y, z, c)), device(x, y, z, c))
        for y in range(NY)
        for z in range(NZ)
        for c in range(NC)
        for x in range(NX)
    ]
    return lax.ppermute(value, AXES, pairs)


def from_x(value, k):
    return fetched(value, lambda x, y, z, c: (x + k, y, z, c))


def from_y(value, k):
    return fetched(value, lambda x, y, z, c: (x, y + k, z, c))


PLANES = [[device(x, y, z, c) for x in range(NX) for y in range(NY)] for z in range(NZ) for c in range(NC)]
MEMBERS = 16


def exchanged(value, groups):
    return lax.all_to_all(value, AXES, 0, 0, axis_index_groups=groups, tiled=True)


def from_core(value):
    return fetched(value, lambda x, y, z, c: (x, y, z, c + 1))


def three_parts(v):
    high = v.astype(bf16).astype(f32)
    rest = v - high
    middle = rest.astype(bf16).astype(f32)
    return high, middle, rest - middle


def place():
    own, x = lax.axis_index("own"), lax.axis_index("split")
    return x, own // (NZ * NC), (own // NC) % NZ, own % NC


def target_owners():
    x, y, z, c = place()
    row = y * (NZ * NC)
    near = row + ((z + x) % NZ) * NC
    far = row + ((z + x + NZ // 2) % NZ) * NC
    return near + c, near + 1 - c, far + c, far + 1 - c


def centre(ref):
    middle = jnp.mean(ref[0], axis=1, keepdims=True)
    return jnp.broadcast_to(middle, (PACKED, CELLS))


def load_cluster(ref, a, middle):
    top = ref[a, 0:48, :] - middle[0:48]
    tail = ref[a, 48:PACKED, :]
    row = lax.broadcasted_iota(jnp.int32, (8, CELLS), 0)
    extra = tail[2:3, :]
    tail = jnp.where(row < 2, tail - middle[48:56], 0.0)
    square = jnp.sum(top * top, axis=0, keepdims=True) + jnp.sum(tail * tail, axis=0, keepdims=True)
    return top, tail, extra, square


def with_rows(tail, first, second):
    row = lax.broadcasted_iota(jnp.int32, (8, CELLS), 0)
    for k in range(3):
        tail = jnp.where(row == 2 + k, first[k], tail)
        tail = jnp.where(row == 5 + k, second[k], tail)
    return tail


def store_operand(ref, n, top, tail, first, second):
    zeros = jnp.zeros((8, CELLS), f32)
    for part, (head, end) in enumerate(zip(three_parts(top)[:2], three_parts(tail)[:2])):
        end = with_rows(end, first, second) if part == 0 else end
        at = part * BLOCK
        ref[n, at : at + 48, :] = head.astype(bf16)
        ref[n, at + 48 : at + BLOCK, :] = jnp.concatenate([end, zeros], axis=0).astype(bf16)


def logsum(top, total):
    return jnp.where(total > 0.0, top + jnp.log2(total), NEGATIVE)


def merged(parts):
    top = parts[0]
    for part in parts[1:]:
        top = jnp.maximum(top, part)
    total = sum(jnp.exp2(part - top) for part in parts)
    return top + jnp.log2(total)


def over_pairs(count, list_ref, left_ref, right_ref, pick, top_ref, sum_ref, scores, tops):
    def multiply(n, k):
        pair = list_ref[n]
        left, right, _ = pick(pair >> 8, pair & 255)
        cells = left_ref[left]
        high, low = right_ref[right, 0:BLOCK, :], right_ref[right, BLOCK:DEPTH, :]
        e = jnp.dot(
            jnp.concatenate([cells, cells], axis=1),
            jnp.concatenate([high, high, low, low], axis=0),
            preferred_element_type=f32,
        )
        scores[k][...] = e
        tops[k][...] = jnp.max(e.reshape(CELLS // 8, 8, CELLS), axis=0)

    def absorb(n, k):
        pair = list_ref[n]
        _, _, place = pick(pair >> 8, pair & 255)
        top = tops[k][...]
        e = scores[k][...].reshape(CELLS // 8, 8, CELLS)
        total = jnp.sum(jnp.exp2(e - top[None]), axis=0)
        old = top_ref[place]
        new = jnp.maximum(old, top)
        sum_ref[place] = sum_ref[place] * jnp.exp2(old - new) + total * jnp.exp2(top - new)
        top_ref[place] = new

    def step(q, carry):
        absorb(4 * q + 0, 0)
        multiply(4 * q + 4, 0)
        absorb(4 * q + 1, 1)
        multiply(4 * q + 5, 1)
        absorb(4 * q + 2, 2)
        multiply(4 * q + 6, 2)
        absorb(4 * q + 3, 3)
        multiply(4 * q + 7, 3)
        return carry

    multiply(0, 0)
    multiply(1, 1)
    multiply(2, 2)
    multiply(3, 3)
    lax.fori_loop(0, (count + 3) // 4, step, 0)


def finish(top_ref, sum_ref):
    tops, sums = top_ref[0 : 4 * CL], sum_ref[0 : 4 * CL]
    top = jnp.max(tops, axis=1, keepdims=True)
    total = jnp.sum(sums * jnp.exp2(tops - top), axis=1)
    return logsum(top[:, 0, :], total)


def pack_kernel(cells_in, extra_in, more_cells_in, more_extra_in, out, more_out, cells, more_cells, extra, more_extra, sem):
    copies = [
        pltpu.make_async_copy(a, b, sem.at[k])
        for k, (a, b) in enumerate(
            (
                (cells_in, cells),
                (extra_in, extra),
                (more_cells_in, more_cells),
                (more_extra_in, more_extra),
            )
        )
    ]
    for copy in copies:
        copy.start()
    for k, (a, b, o) in enumerate(((cells, extra, out), (more_cells, more_extra, more_out))):
        copies[2 * k].wait()
        copies[2 * k + 1].wait()
        for n in range(CL):
            o[n, 0:COMP, :] = a[:, n, :]
            o[n, COMP : COMP + 1, :] = b[n : n + 1, :]
            o[n, COMP + 1 : PACKED, :] = jnp.zeros((PACKED - COMP - 1, CELLS), f32)


def row_kernel(codes_in, s0, s1, s2, s3, t0, t1, t2, t3, out, list_out, xn, yn, mass, square_out, codes, list_ref, yt, top, tot, *rest):
    scores, tops, sem = rest[:DEEP], rest[DEEP : 2 * DEEP], rest[2 * DEEP]
    arriving = pltpu.make_async_copy(codes_in, codes, sem.at[0])
    arriving.start()
    one = jnp.ones((1, CELLS), f32)
    ones = (one, one, one)
    middle = centre(s0)
    for k, ref in enumerate((s0, s1, s2, s3)):
        for a in range(CL):
            head, tail, extra, square = load_cluster(ref, a, middle)
            mass[k * CL + a : k * CL + a + 1, :] = extra
            square_out[k * CL + a : k * CL + a + 1, :] = square
            weight = three_parts(-square * SCALE)
            store_operand(xn, k * CL + a, head * (2.0 * SCALE), tail * (2.0 * SCALE), weight, ones)
    top[...] = jnp.full(top.shape, NEGATIVE, f32)
    tot[...] = jnp.zeros(tot.shape, f32)
    arriving.wait()
    owners = target_owners()
    count = jnp.int32(0)
    y = place()[1]
    for k in range(4):
        for d in range(NX):
            for t in range(4):
                code = codes[d * NY + (y + k) % NY, owners[t]]
                source = k * CL + (code >> 2)
                list_ref[count] = source * 256 + t * CL + (code & 3)
                count = count + (code >= 0).astype(jnp.int32)
    for k in range(2 * DEEP):
        list_ref[count + k] = 4 * CL * 256
    list_ref[LIST - 1] = count
    leaving = pltpu.make_async_copy(list_ref, list_out, sem.at[1])
    leaving.start()
    xn[4 * CL] = jnp.zeros((DEPTH, CELLS), bf16)
    for k, ref in enumerate((t0, t1, t2, t3)):
        for a in range(CL):
            head, tail, prior, square = load_cluster(ref, a, middle)
            weight = three_parts((prior - square) * SCALE)
            store_operand(yn, k * CL + a, head, tail, ones, weight)
            yt[k * CL + a] = yn[k * CL + a].T
    over_pairs(count, list_ref, yt, xn, lambda s, t: (t, s, s), top, tot, scores, tops)
    rows = finish(top, tot).reshape(4, CL, CELLS)
    for k in range(4):
        for m in range(MEMBERS):
            out[m, (y + k) % NY] = rows[k]
    leaving.wait()


def column_kernel(list_in, came, mass, square, x_in, yn, kept, given, potential, list_ref, xn, xt, four, top, tot, *rest):
    scores, tops, sem = rest[:DEEP], rest[DEEP : 2 * DEEP], rest[2 * DEEP]
    arriving = pltpu.make_async_copy(list_in, list_ref, sem.at[0])
    arriving.start()
    y = place()[1]
    four[...] = merged([came[m] for m in range(MEMBERS)])
    row = lax.broadcasted_iota(jnp.int32, (16, CELLS), 0)
    for k in range(4):
        rows = four[(y + k) % NY]
        for a in range(CL):
            n = k * CL + a
            p = EPSILON * mass[n : n + 1, :] - (EPSILON * LN2) * rows[a : a + 1]
            if k == 0:
                potential[a : a + 1, :] = p
            weight = three_parts((p - square[n : n + 1, :]) * SCALE)
            xn[...] = x_in[n]
            end = xn[48:64, :].astype(f32)
            for part in range(3):
                end = jnp.where(row == 2 + part, weight[part], end)
            xn[48:64, :] = end.astype(bf16)
            xt[n] = xn[...].T
    xt[4 * CL] = jnp.zeros((CELLS, DEPTH), bf16)
    top[...] = jnp.full(top.shape, NEGATIVE, f32)
    tot[...] = jnp.zeros(tot.shape, f32)
    arriving.wait()

    def pick(s, t):
        return s, t, jnp.where(s == 4 * CL, 4 * CL, t)

    over_pairs(list_ref[LIST - 1], list_ref, xt, yn, pick, top, tot, scores, tops)
    columns = finish(top, tot)
    for k in range(2):
        kept[k * CL : (k + 1) * CL, :] = columns[2 * k * CL : (2 * k + 1) * CL]
        given[k * CL : (k + 1) * CL, :] = columns[(2 * k + 1) * CL : (2 * k + 2) * CL]


VMEM = pl.BlockSpec(memory_space=pltpu.VMEM)
ANY = pl.BlockSpec(memory_space=pl.ANY)
HBM = pl.BlockSpec(memory_space=pltpu.HBM)


def work(source_coords, target_coords, source_logmass, target_logmass, target_prior, pair_source, pair_target):
    codes = pair_source * 4 + pair_target
    codes = jnp.where(pair_target >= 0, codes, -1).reshape(1, -1)
    codes = exchanged(jnp.broadcast_to(codes, (MEMBERS, codes.shape[1])), PLANES)

    cells = jax.ShapeDtypeStruct((CL, PACKED, CELLS), f32)
    loose = pltpu.VMEM((COMP, CL, CELLS), f32)
    t, s0 = pl.pallas_call(
        pack_kernel,
        out_shape=(cells, cells),
        in_specs=[HBM] * 4,
        out_specs=(VMEM, VMEM),
        scratch_shapes=[loose, loose] + [pltpu.VMEM((CL, CELLS), f32)] * 2 + [pltpu.SemaphoreType.DMA((4,))],
        compiler_params=pltpu.CompilerParams(vmem_limit_bytes=4 * 2**20),
        name="pack",
    )(
        *(
            pltpu.with_memory_space_constraint(value, pltpu.HBM)
            for value in (
                jnp.transpose(target_coords, (1, 0, 2)),
                target_prior,
                jnp.transpose(source_coords, (1, 0, 2)),
                source_logmass,
            )
        )
    )
    t2 = fetched(t, lambda x, y, z, c: (x, y, z + x + FAR, c))
    t0 = fetched(t, lambda x, y, z, c: (x, y, z + x, c))
    s1, s2, s3 = (from_y(s0, k) for k in (1, 2, 3))
    t1, t3 = from_core(t0), from_core(t2)
    shards = (s0, s1, s2, s3, t0, t1, t2, t3)

    shared = (
        [pltpu.VMEM((4 * CL + 1, 8, CELLS), f32)] * 2
        + [pltpu.VMEM((CELLS, CELLS), f32)] * DEEP
        + [pltpu.VMEM((8, CELLS), f32)] * DEEP
        + [pltpu.SemaphoreType.DMA((2,))]
    )
    params = pltpu.CompilerParams(vmem_limit_bytes=16 * 2**20)
    rows, pairs, xn, yn, mass, square = pl.pallas_call(
        row_kernel,
        out_shape=(
            jax.ShapeDtypeStruct((MEMBERS, 4, CL, CELLS), f32),
            jax.ShapeDtypeStruct((LIST,), jnp.int32),
            jax.ShapeDtypeStruct((4 * CL + 1, DEPTH, CELLS), bf16),
            jax.ShapeDtypeStruct((4 * CL, DEPTH, CELLS), bf16),
            jax.ShapeDtypeStruct((4 * CL, CELLS), f32),
            jax.ShapeDtypeStruct((4 * CL, CELLS), f32),
        ),
        in_specs=[ANY] + [VMEM] * 8,
        out_specs=(VMEM, ANY, VMEM, VMEM, VMEM, VMEM),
        scratch_shapes=[
            pltpu.SMEM((MEMBERS, SLOTS), jnp.int32),
            pltpu.SMEM((LIST,), jnp.int32),
            pltpu.VMEM((4 * CL, CELLS, DEPTH), bf16),
        ]
        + shared,
        compiler_params=params,
        name="rows",
    )(codes, *shards)

    rows = exchanged(rows, PLANES)

    kept, given, source_potential = pl.pallas_call(
        column_kernel,
        out_shape=(
            jax.ShapeDtypeStruct((2 * CL, CELLS), f32),
            jax.ShapeDtypeStruct((2 * CL, CELLS), f32),
            jax.ShapeDtypeStruct((CL, CELLS), f32),
        ),
        in_specs=[ANY] + [VMEM] * 5,
        out_specs=(VMEM, VMEM, VMEM),
        scratch_shapes=[
            pltpu.SMEM((LIST,), jnp.int32),
            pltpu.VMEM((DEPTH, CELLS), bf16),
            pltpu.VMEM((4 * CL + 1, CELLS, DEPTH), bf16),
            pltpu.VMEM((4, CL, CELLS), f32),
        ]
        + shared,
        compiler_params=params,
        name="columns",
    )(pairs, rows, mass, square, xn, yn)

    kept = merged([kept, from_core(given)])
    first = fetched(kept[:CL], lambda x, y, z, c: (x, y, z - x, c))
    second = fetched(kept[CL:], lambda x, y, z, c: (x, y, z - x - FAR, c))
    part = merged([first, second])
    part = merged([part] + [from_x(part, k) for k in (1, 2, 3)])
    target_potential = EPSILON * target_logmass + target_prior - (EPSILON * LN2) * part
    return source_potential, target_potential


def solution(mesh):
    return jax.shard_map(
        work,
        mesh=mesh,
        in_specs=(
            P("own", None, None),
            P("own", None, None),
            P("own", None),
            P("own", None),
            P("own", None),
            P("own", "split", None, None),
            P("own", "split", None, None),
        ),
        out_specs=(P("own", None), P("own", None)),
        check_vma=False,
    )
```

```python
import math

import jax
import jax.numpy as jnp
from jax import lax
from jax.experimental import pallas as pl
from jax.experimental.pallas import tpu as pltpu
from jax.sharding import PartitionSpec as P


EPSILON = 0.5
NEGATIVE = -1e30
LN2 = math.log(2.0)
SCALE = 1.0 / (EPSILON * LN2)

COMP = 50
CL = 4
CELLS = 256
PACKED = 52
NY, NZ, NC, NX = 4, 8, 2, 4
AXES = ("own", "split")

FAR = NZ // 2

BLOCK = 64
DEPTH = 2 * BLOCK
SLOTS = 64
DEEP = 4
LIST = SLOTS + 16

f32, bf16 = jnp.float32, jnp.bfloat16


def device(x, y, z, c):
    return (((y % NY) * NZ + z % NZ) * NC + c % NC) * NX + x % NX


def fetched(value, source):
    pairs = [
        (device(*source(x, y, z, c)), device(x, y, z, c))
        for y in range(NY)
        for z in range(NZ)
        for c in range(NC)
        for x in range(NX)
    ]
    return lax.ppermute(value, AXES, pairs)


def from_x(value, k):
    return fetched(value, lambda x, y, z, c: (x + k, y, z, c))


def from_y(value, k):
    return fetched(value, lambda x, y, z, c: (x, y + k, z, c))


PLANES = [[device(x, y, z, c) for x in range(NX) for y in range(NY)] for z in range(NZ) for c in range(NC)]
MEMBERS = 16


def exchanged(value, groups):
    return lax.all_to_all(value, AXES, 0, 0, axis_index_groups=groups, tiled=True)


def from_core(value):
    return fetched(value, lambda x, y, z, c: (x, y, z, c + 1))


def three_parts(v):
    high = v.astype(bf16).astype(f32)
    rest = v - high
    middle = rest.astype(bf16).astype(f32)
    return high, middle, rest - middle


def place():
    own, x = lax.axis_index("own"), lax.axis_index("split")
    return x, own // (NZ * NC), (own // NC) % NZ, own % NC


def target_owners():
    x, y, z, c = place()
    row = y * (NZ * NC)
    near = row + ((z + x) % NZ) * NC
    far = row + ((z + x + NZ // 2) % NZ) * NC
    return near + c, near + 1 - c, far + c, far + 1 - c


def centre(ref):
    middle = jnp.mean(ref[0:56, :], axis=1, keepdims=True)
    return jnp.broadcast_to(middle, (56, CELLS))


def load_cluster(ref, a, middle):
    at = PACKED * a
    top = ref[at : at + 48, :] - middle[0:48]
    tail = jnp.concatenate([ref[at + 48 : at + PACKED, :], jnp.zeros((4, CELLS), f32)], axis=0)
    row = lax.broadcasted_iota(jnp.int32, (8, CELLS), 0)
    extra = tail[2:3, :]
    tail = jnp.where(row < 2, tail - middle[48:56], 0.0)
    square = jnp.sum(top * top, axis=0, keepdims=True) + jnp.sum(tail * tail, axis=0, keepdims=True)
    return top, tail, extra, square


def with_rows(tail, first, second):
    row = lax.broadcasted_iota(jnp.int32, (8, CELLS), 0)
    for k in range(3):
        tail = jnp.where(row == 2 + k, first[k], tail)
        tail = jnp.where(row == 5 + k, second[k], tail)
    return tail


def store_operand(ref, n, top, tail, first, second):
    zeros = jnp.zeros((8, CELLS), f32)
    for part, (head, end) in enumerate(zip(three_parts(top)[:2], three_parts(tail)[:2])):
        end = with_rows(end, first, second) if part == 0 else end
        at = part * BLOCK
        ref[n, at : at + 48, :] = head.astype(bf16)
        ref[n, at + 48 : at + BLOCK, :] = jnp.concatenate([end, zeros], axis=0).astype(bf16)


def logsum(top, total):
    return jnp.where(total > 0.0, top + jnp.log2(total), NEGATIVE)


def merged(parts):
    top = parts[0]
    for part in parts[1:]:
        top = jnp.maximum(top, part)
    total = sum(jnp.exp2(part - top) for part in parts)
    return top + jnp.log2(total)


def over_pairs(count, list_ref, left_ref, right_ref, pick, top_ref, sum_ref, scores, tops):
    def multiply(n, k):
        pair = list_ref[n]
        left, right, _ = pick(pair >> 8, pair & 255)
        cells = left_ref[left]
        high, low = right_ref[right, 0:BLOCK, :], right_ref[right, BLOCK:DEPTH, :]
        e = jnp.dot(
            jnp.concatenate([cells, cells], axis=1),
            jnp.concatenate([high, high, low, low], axis=0),
            preferred_element_type=f32,
        )
        scores[k][...] = e
        tops[k][...] = jnp.max(e.reshape(CELLS // 8, 8, CELLS), axis=0)

    def absorb(n, k):
        pair = list_ref[n]
        _, _, place = pick(pair >> 8, pair & 255)
        top = tops[k][...]
        e = scores[k][...].reshape(CELLS // 8, 8, CELLS)
        total = jnp.sum(jnp.exp2(e - top[None]), axis=0)
        old = top_ref[place]
        new = jnp.maximum(old, top)
        sum_ref[place] = sum_ref[place] * jnp.exp2(old - new) + total * jnp.exp2(top - new)
        top_ref[place] = new

    def step(q, carry):
        absorb(4 * q + 0, 0)
        multiply(4 * q + 4, 0)
        absorb(4 * q + 1, 1)
        multiply(4 * q + 5, 1)
        absorb(4 * q + 2, 2)
        multiply(4 * q + 6, 2)
        absorb(4 * q + 3, 3)
        multiply(4 * q + 7, 3)
        return carry

    multiply(0, 0)
    multiply(1, 1)
    multiply(2, 2)
    multiply(3, 3)
    lax.fori_loop(0, (count + 3) // 4, step, 0)


def finish(top_ref, sum_ref):
    tops, sums = top_ref[0 : 4 * CL], sum_ref[0 : 4 * CL]
    top = jnp.max(tops, axis=1, keepdims=True)
    total = jnp.sum(sums * jnp.exp2(tops - top), axis=1)
    return logsum(top[:, 0, :], total)


def pack_kernel(cells_in, extra_in, more_cells_in, more_extra_in, source_in, target_in, out, more_out, codes_out, cells, more_cells, extra, more_extra, source, target, sem):
    copies = [
        pltpu.make_async_copy(a, b, sem.at[k])
        for k, (a, b) in enumerate(
            (
                (cells_in, cells),
                (extra_in, extra),
                (more_cells_in, more_cells),
                (more_extra_in, more_extra),
                (source_in, source),
                (target_in, target),
            )
        )
    ]
    for copy in copies:
        copy.start()
    for k, (a, b, o) in enumerate(((cells, extra, out), (more_cells, more_extra, more_out))):
        copies[2 * k].wait()
        copies[2 * k + 1].wait()
        if k == 1:
            copies[4].wait()
            copies[5].wait()
            codes = jnp.where(target[...] >= 0, source[...] * CL + target[...], -1)
            codes_out[...] = jnp.broadcast_to(codes[None], codes_out.shape)
        for n in range(CL):
            at = PACKED * n
            o[at : at + COMP, :] = a[:, n, :]
            o[at + COMP : at + COMP + 1, :] = b[n : n + 1, :]
            o[at + COMP + 1 : at + PACKED, :] = jnp.zeros((PACKED - COMP - 1, CELLS), f32)


def row_kernel(codes_in, s0, s1, s2, s3, t0, t1, t2, t3, out, list_out, xn, yn, mass, square_out, codes, list_ref, yt, top, tot, *rest):
    scores, tops, sem = rest[:DEEP], rest[DEEP : 2 * DEEP], rest[2 * DEEP]
    arriving = pltpu.make_async_copy(codes_in, codes, sem.at[0])
    arriving.start()
    one = jnp.ones((1, CELLS), f32)
    ones = (one, one, one)
    middle = centre(s0)
    for k, ref in enumerate((s0, s1, s2, s3)):
        for a in range(CL):
            head, tail, extra, square = load_cluster(ref, a, middle)
            mass[k * CL + a : k * CL + a + 1, :] = extra
            square_out[k * CL + a : k * CL + a + 1, :] = square
            weight = three_parts(-square * SCALE)
            store_operand(xn, k * CL + a, head * (2.0 * SCALE), tail * (2.0 * SCALE), weight, ones)
    top[...] = jnp.full(top.shape, NEGATIVE, f32)
    tot[...] = jnp.zeros(tot.shape, f32)
    arriving.wait()
    owners = target_owners()
    count = jnp.int32(0)
    y = place()[1]
    for k in range(4):
        for d in range(NX):
            for t in range(4):
                code = codes[d * NY + (y + k) % NY, owners[t]]
                source = k * CL + (code >> 2)
                list_ref[count] = source * 256 + t * CL + (code & 3)
                count = count + (code >= 0).astype(jnp.int32)
    for k in range(2 * DEEP):
        list_ref[count + k] = 4 * CL * 256
    list_ref[LIST - 1] = count
    leaving = pltpu.make_async_copy(list_ref, list_out, sem.at[1])
    leaving.start()
    xn[4 * CL] = jnp.zeros((DEPTH, CELLS), bf16)
    for k, ref in enumerate((t0, t1, t2, t3)):
        for a in range(CL):
            head, tail, prior, square = load_cluster(ref, a, middle)
            weight = three_parts((prior - square) * SCALE)
            store_operand(yn, k * CL + a, head, tail, ones, weight)
            yt[k * CL + a] = yn[k * CL + a].T
    over_pairs(count, list_ref, yt, xn, lambda s, t: (t, s, s), top, tot, scores, tops)
    out[...] = finish(top, tot)
    leaving.wait()


def column_kernel(list_in, m0, m1, m2, m3, mass, square, x_in, yn, kept, given, potential, list_ref, xn, xt, top, tot, *rest):
    scores, tops, sem = rest[:DEEP], rest[DEEP : 2 * DEEP], rest[2 * DEEP]
    arriving = pltpu.make_async_copy(list_in, list_ref, sem.at[0])
    arriving.start()
    came = [m[...].reshape(4, CL, CELLS) for m in (m0, m1, m2, m3)]
    row = lax.broadcasted_iota(jnp.int32, (16, CELLS), 0)
    for k in range(4):
        rows = merged([came[d][(k - d) % NY] for d in range(NY)])
        for a in range(CL):
            n = k * CL + a
            p = EPSILON * mass[n : n + 1, :] - (EPSILON * LN2) * rows[a : a + 1]
            if k == 0:
                potential[a : a + 1, :] = p
            weight = three_parts((p - square[n : n + 1, :]) * SCALE)
            xn[...] = x_in[n]
            end = xn[48:64, :].astype(f32)
            for part in range(3):
                end = jnp.where(row == 2 + part, weight[part], end)
            xn[48:64, :] = end.astype(bf16)
            xt[n] = xn[...].T
    xt[4 * CL] = jnp.zeros((CELLS, DEPTH), bf16)
    top[...] = jnp.full(top.shape, NEGATIVE, f32)
    tot[...] = jnp.zeros(tot.shape, f32)
    arriving.wait()

    def pick(s, t):
        return s, t, jnp.where(s == 4 * CL, 4 * CL, t)

    over_pairs(list_ref[LIST - 1], list_ref, xt, yn, pick, top, tot, scores, tops)
    columns = finish(top, tot)
    for k in range(2):
        kept[k * CL : (k + 1) * CL, :] = columns[2 * k * CL : (2 * k + 1) * CL]
        given[k * CL : (k + 1) * CL, :] = columns[(2 * k + 1) * CL : (2 * k + 2) * CL]


VMEM = pl.BlockSpec(memory_space=pltpu.VMEM)
ANY = pl.BlockSpec(memory_space=pl.ANY)
HBM = pl.BlockSpec(memory_space=pltpu.HBM)


def work(source_coords, target_coords, source_logmass, target_logmass, target_prior, pair_source, pair_target):
    cells = jax.ShapeDtypeStruct((CL * PACKED, CELLS), f32)
    loose = pltpu.VMEM((COMP, CL, CELLS), f32)
    t, s0, codes = pl.pallas_call(
        pack_kernel,
        out_shape=(cells, cells, jax.ShapeDtypeStruct((MEMBERS, 1, SLOTS), jnp.int32)),
        in_specs=[HBM] * 6,
        out_specs=(VMEM, VMEM, VMEM),
        scratch_shapes=[loose, loose]
        + [pltpu.VMEM((CL, CELLS), f32)] * 2
        + [pltpu.VMEM((1, SLOTS), jnp.int32)] * 2
        + [pltpu.SemaphoreType.DMA((6,))],
        compiler_params=pltpu.CompilerParams(vmem_limit_bytes=4 * 2**20),
        name="pack",
    )(
        *(
            pltpu.with_memory_space_constraint(value, pltpu.HBM)
            for value in (
                jnp.transpose(target_coords, (1, 0, 2)),
                target_prior,
                jnp.transpose(source_coords, (1, 0, 2)),
                source_logmass,
                pair_source.reshape(1, SLOTS),
                pair_target.reshape(1, SLOTS),
            )
        )
    )
    t2 = fetched(t, lambda x, y, z, c: (x, y, z + x + FAR, c))
    t0 = fetched(t, lambda x, y, z, c: (x, y, z + x, c))
    s1, s2, s3 = (from_y(s0, k) for k in (1, 2, 3))
    codes = exchanged(codes, PLANES).reshape(MEMBERS, SLOTS)
    t1, t3 = from_core(t0), from_core(t2)
    shards = (s0, s1, s2, s3, t0, t1, t2, t3)

    shared = (
        [pltpu.VMEM((4 * CL + 1, 8, CELLS), f32)] * 2
        + [pltpu.VMEM((CELLS, CELLS), f32)] * DEEP
        + [pltpu.VMEM((8, CELLS), f32)] * DEEP
        + [pltpu.SemaphoreType.DMA((2,))]
    )
    params = pltpu.CompilerParams(vmem_limit_bytes=16 * 2**20)
    rows, pairs, xn, yn, mass, square = pl.pallas_call(
        row_kernel,
        out_shape=(
            jax.ShapeDtypeStruct((4 * CL, CELLS), f32),
            jax.ShapeDtypeStruct((LIST,), jnp.int32),
            jax.ShapeDtypeStruct((4 * CL + 1, DEPTH, CELLS), bf16),
            jax.ShapeDtypeStruct((4 * CL, DEPTH, CELLS), bf16),
            jax.ShapeDtypeStruct((4 * CL, CELLS), f32),
            jax.ShapeDtypeStruct((4 * CL, CELLS), f32),
        ),
        in_specs=[ANY] + [VMEM] * 8,
        out_specs=(VMEM, ANY, VMEM, VMEM, VMEM, VMEM),
        scratch_shapes=[
            pltpu.SMEM((MEMBERS, SLOTS), jnp.int32),
            pltpu.SMEM((LIST,), jnp.int32),
            pltpu.VMEM((4 * CL, CELLS, DEPTH), bf16),
        ]
        + shared,
        compiler_params=params,
        name="rows",
    )(codes, *shards)

    rows = merged([rows] + [from_x(rows, k) for k in (1, 2, 3)])
    others = [from_y(rows, k) for k in (1, 2, 3)]

    kept, given, source_potential = pl.pallas_call(
        column_kernel,
        out_shape=(
            jax.ShapeDtypeStruct((2 * CL, CELLS), f32),
            jax.ShapeDtypeStruct((2 * CL, CELLS), f32),
            jax.ShapeDtypeStruct((CL, CELLS), f32),
        ),
        in_specs=[ANY] + [VMEM] * 8,
        out_specs=(VMEM, VMEM, VMEM),
        scratch_shapes=[
            pltpu.SMEM((LIST,), jnp.int32),
            pltpu.VMEM((DEPTH, CELLS), bf16),
            pltpu.VMEM((4 * CL + 1, CELLS, DEPTH), bf16),
        ]
        + shared,
        compiler_params=params,
        name="columns",
    )(pairs, rows, *others, mass, square, xn, yn)

    kept = merged([kept, from_core(given)])
    first = fetched(kept[:CL], lambda x, y, z, c: (x, y, z - x, c))
    second = fetched(kept[CL:], lambda x, y, z, c: (x, y, z - x - FAR, c))
    part = merged([first, second])
    part = merged([part] + [from_x(part, k) for k in (1, 2, 3)])
    target_potential = EPSILON * target_logmass + target_prior - (EPSILON * LN2) * part
    return source_potential, target_potential


def solution(mesh):
    return jax.shard_map(
        work,
        mesh=mesh,
        in_specs=(
            P("own", None, None),
            P("own", None, None),
            P("own", None),
            P("own", None),
            P("own", None),
            P("own", "split", None, None),
            P("own", "split", None, None),
        ),
        out_specs=(P("own", None), P("own", None)),
        check_vma=False,
    )
```

```python
import math

import jax
import jax.numpy as jnp
from jax import lax
from jax.experimental import pallas as pl
from jax.experimental.pallas import tpu as pltpu
from jax.sharding import PartitionSpec as P


EPSILON = 0.5
NEGATIVE = -1e30
LN2 = math.log(2.0)
SCALE = 1.0 / (EPSILON * LN2)

COMP = 50
CL = 4
CELLS = 256
PACKED = 52
NY, NZ, NC, NX = 4, 8, 2, 4
AXES = ("own", "split")

FAR = NZ // 2

BLOCK = 64
DEPTH = 2 * BLOCK
SLOTS = 64
DEEP = 4
LIST = SLOTS + 16

f32, bf16 = jnp.float32, jnp.bfloat16


def device(x, y, z, c):
    return (((y % NY) * NZ + z % NZ) * NC + c % NC) * NX + x % NX


def fetched(value, source):
    pairs = [
        (device(*source(x, y, z, c)), device(x, y, z, c))
        for y in range(NY)
        for z in range(NZ)
        for c in range(NC)
        for x in range(NX)
    ]
    return lax.ppermute(value, AXES, pairs)


def from_x(value, k):
    return fetched(value, lambda x, y, z, c: (x + k, y, z, c))


def from_y(value, k):
    return fetched(value, lambda x, y, z, c: (x, y + k, z, c))


PLANES = [[device(x, y, z, c) for x in range(NX) for y in range(NY)] for z in range(NZ) for c in range(NC)]
MEMBERS = 16


def exchanged(value, groups):
    return lax.all_to_all(value, AXES, 0, 0, axis_index_groups=groups, tiled=True)


def from_core(value):
    return fetched(value, lambda x, y, z, c: (x, y, z, c + 1))


def three_parts(v):
    high = v.astype(bf16).astype(f32)
    rest = v - high
    middle = rest.astype(bf16).astype(f32)
    return high, middle, rest - middle


def place():
    own, x = lax.axis_index("own"), lax.axis_index("split")
    return x, own // (NZ * NC), (own // NC) % NZ, own % NC


def target_owners():
    x, y, z, c = place()
    row = y * (NZ * NC)
    near = row + ((z + x) % NZ) * NC
    far = row + ((z + x + NZ // 2) % NZ) * NC
    return near + c, near + 1 - c, far + c, far + 1 - c


def centre(ref):
    middle = jnp.mean(ref[0:56, :], axis=1, keepdims=True)
    return jnp.broadcast_to(middle, (56, CELLS))


def load_cluster(ref, a, middle):
    at = PACKED * a
    top = ref[at : at + 48, :] - middle[0:48]
    tail = jnp.concatenate([ref[at + 48 : at + PACKED, :], jnp.zeros((4, CELLS), f32)], axis=0)
    row = lax.broadcasted_iota(jnp.int32, (8, CELLS), 0)
    extra = tail[2:3, :]
    tail = jnp.where(row < 2, tail - middle[48:56], 0.0)
    square = jnp.sum(top * top, axis=0, keepdims=True) + jnp.sum(tail * tail, axis=0, keepdims=True)
    return top, tail, extra, square


def with_rows(tail, first, second):
    row = lax.broadcasted_iota(jnp.int32, (8, CELLS), 0)
    for k in range(3):
        tail = jnp.where(row == 2 + k, first[k], tail)
        tail = jnp.where(row == 5 + k, second[k], tail)
    return tail


def store_operand(ref, n, top, tail, first, second):
    zeros = jnp.zeros((8, CELLS), f32)
    for part, (head, end) in enumerate(zip(three_parts(top)[:2], three_parts(tail)[:2])):
        end = with_rows(end, first, second) if part == 0 else end
        at = part * BLOCK
        ref[n, at : at + 48, :] = head.astype(bf16)
        ref[n, at + 48 : at + BLOCK, :] = jnp.concatenate([end, zeros], axis=0).astype(bf16)


def logsum(top, total):
    return jnp.where(total > 0.0, top + jnp.log2(total), NEGATIVE)


def merged(parts):
    top = parts[0]
    for part in parts[1:]:
        top = jnp.maximum(top, part)
    total = sum(jnp.exp2(part - top) for part in parts)
    return top + jnp.log2(total)


def over_pairs(count, list_ref, left_ref, right_ref, pick, top_ref, sum_ref, scores, tops):
    def multiply(n, k):
        pair = list_ref[n]
        left, right, _ = pick(pair >> 8, pair & 255)
        cells = left_ref[left]
        high, low = right_ref[right, 0:BLOCK, :], right_ref[right, BLOCK:DEPTH, :]
        e = jnp.dot(
            jnp.concatenate([cells, cells], axis=1),
            jnp.concatenate([high, high, low, low], axis=0),
            preferred_element_type=f32,
        )
        scores[k][...] = e
        tops[k][...] = jnp.max(e.reshape(CELLS // 8, 8, CELLS), axis=0)

    def absorb(n, k):
        pair = list_ref[n]
        _, _, place = pick(pair >> 8, pair & 255)
        top = tops[k][...]
        e = scores[k][...].reshape(CELLS // 8, 8, CELLS)
        total = jnp.sum(jnp.exp2(e - top[None]), axis=0)
        old = top_ref[place]
        new = jnp.maximum(old, top)
        sum_ref[place] = sum_ref[place] * jnp.exp2(old - new) + total * jnp.exp2(top - new)
        top_ref[place] = new

    def step(q, carry):
        absorb(4 * q + 0, 0)
        multiply(4 * q + 4, 0)
        absorb(4 * q + 1, 1)
        multiply(4 * q + 5, 1)
        absorb(4 * q + 2, 2)
        multiply(4 * q + 6, 2)
        absorb(4 * q + 3, 3)
        multiply(4 * q + 7, 3)
        return carry

    multiply(0, 0)
    multiply(1, 1)
    multiply(2, 2)
    multiply(3, 3)
    lax.fori_loop(0, (count + 3) // 4, step, 0)


def finish(top_ref, sum_ref):
    tops, sums = top_ref[0 : 4 * CL], sum_ref[0 : 4 * CL]
    top = jnp.max(tops, axis=1, keepdims=True)
    total = jnp.sum(sums * jnp.exp2(tops - top), axis=1)
    return logsum(top[:, 0, :], total)


def pack_kernel(cells_in, extra_in, more_cells_in, more_extra_in, source_in, target_in, out, more_out, codes_out, cells, more_cells, extra, more_extra, source, target, sem):
    copies = [
        pltpu.make_async_copy(a, b, sem.at[k])
        for k, (a, b) in enumerate(
            (
                (cells_in, cells),
                (extra_in, extra),
                (more_cells_in, more_cells),
                (more_extra_in, more_extra),
                (source_in, source),
                (target_in, target),
            )
        )
    ]
    for copy in (*copies[4:], *copies[:4]):
        copy.start()
    for k, (a, b, o) in enumerate(((cells, extra, out), (more_cells, more_extra, more_out))):
        copies[2 * k].wait()
        copies[2 * k + 1].wait()
        for n in range(CL):
            at = PACKED * n
            o[at : at + COMP, :] = a[:, n, :]
            o[at + COMP : at + COMP + 1, :] = b[n : n + 1, :]
            o[at + COMP + 1 : at + PACKED, :] = jnp.zeros((PACKED - COMP - 1, CELLS), f32)
    copies[4].wait()
    copies[5].wait()
    codes = jnp.where(target[...] >= 0, source[...] * CL + target[...], -1)
    codes_out[...] = jnp.broadcast_to(codes[None], codes_out.shape)


def row_kernel(codes_in, s0, s1, s2, s3, t0, t1, t2, t3, out, list_out, xn, yn, mass, square_out, codes, list_ref, yt, top, tot, *rest):
    scores, tops, sem = rest[:DEEP], rest[DEEP : 2 * DEEP], rest[2 * DEEP]
    arriving = pltpu.make_async_copy(codes_in, codes, sem.at[0])
    arriving.start()
    one = jnp.ones((1, CELLS), f32)
    ones = (one, one, one)
    middle = centre(s0)
    for k, ref in enumerate((s0, s1, s2, s3)):
        for a in range(CL):
            head, tail, extra, square = load_cluster(ref, a, middle)
            mass[k * CL + a : k * CL + a + 1, :] = extra
            square_out[k * CL + a : k * CL + a + 1, :] = square
            weight = three_parts(-square * SCALE)
            store_operand(xn, k * CL + a, head * (2.0 * SCALE), tail * (2.0 * SCALE), weight, ones)
    top[...] = jnp.full(top.shape, NEGATIVE, f32)
    tot[...] = jnp.zeros(tot.shape, f32)
    arriving.wait()
    owners = target_owners()
    count = jnp.int32(0)
    y = place()[1]
    for k in range(4):
        for d in range(NX):
            for t in range(4):
                code = codes[d * NY + (y + k) % NY, owners[t]]
                source = k * CL + (code >> 2)
                list_ref[count] = source * 256 + t * CL + (code & 3)
                count = count + (code >= 0).astype(jnp.int32)
    for k in range(2 * DEEP):
        list_ref[count + k] = 4 * CL * 256
    list_ref[LIST - 1] = count
    leaving = pltpu.make_async_copy(list_ref, list_out, sem.at[1])
    leaving.start()
    xn[4 * CL] = jnp.zeros((DEPTH, CELLS), bf16)
    for k, ref in enumerate((t0, t1, t2, t3)):
        for a in range(CL):
            head, tail, prior, square = load_cluster(ref, a, middle)
            weight = three_parts((prior - square) * SCALE)
            store_operand(yn, k * CL + a, head, tail, ones, weight)
            yt[k * CL + a] = yn[k * CL + a].T
    over_pairs(count, list_ref, yt, xn, lambda s, t: (t, s, s), top, tot, scores, tops)
    rows = finish(top, tot).reshape(4, CL, CELLS)
    for k in range(4):
        for m in range(MEMBERS):
            out[m, (y + k) % NY] = rows[k]
    leaving.wait()


def column_kernel(list_in, came, mass, square, x_in, yn, kept, given, potential, list_ref, xn, xt, four, top, tot, *rest):
    scores, tops, sem = rest[:DEEP], rest[DEEP : 2 * DEEP], rest[2 * DEEP]
    arriving = pltpu.make_async_copy(list_in, list_ref, sem.at[0])
    arriving.start()
    y = place()[1]
    four[...] = merged([came[m] for m in range(MEMBERS)])
    row = lax.broadcasted_iota(jnp.int32, (16, CELLS), 0)
    for k in range(4):
        rows = four[(y + k) % NY]
        for a in range(CL):
            n = k * CL + a
            p = EPSILON * mass[n : n + 1, :] - (EPSILON * LN2) * rows[a : a + 1]
            if k == 0:
                potential[a : a + 1, :] = p
            weight = three_parts((p - square[n : n + 1, :]) * SCALE)
            xn[...] = x_in[n]
            end = xn[48:64, :].astype(f32)
            for part in range(3):
                end = jnp.where(row == 2 + part, weight[part], end)
            xn[48:64, :] = end.astype(bf16)
            xt[n] = xn[...].T
    xt[4 * CL] = jnp.zeros((CELLS, DEPTH), bf16)
    top[...] = jnp.full(top.shape, NEGATIVE, f32)
    tot[...] = jnp.zeros(tot.shape, f32)
    arriving.wait()

    def pick(s, t):
        return s, t, jnp.where(s == 4 * CL, 4 * CL, t)

    over_pairs(list_ref[LIST - 1], list_ref, xt, yn, pick, top, tot, scores, tops)
    columns = finish(top, tot)
    for k in range(2):
        kept[k * CL : (k + 1) * CL, :] = columns[2 * k * CL : (2 * k + 1) * CL]
        given[k * CL : (k + 1) * CL, :] = columns[(2 * k + 1) * CL : (2 * k + 2) * CL]


VMEM = pl.BlockSpec(memory_space=pltpu.VMEM)
ANY = pl.BlockSpec(memory_space=pl.ANY)
HBM = pl.BlockSpec(memory_space=pltpu.HBM)


def work(source_coords, target_coords, source_logmass, target_logmass, target_prior, pair_source, pair_target):
    cells = jax.ShapeDtypeStruct((CL * PACKED, CELLS), f32)
    loose = pltpu.VMEM((COMP, CL, CELLS), f32)
    t, s0, codes = pl.pallas_call(
        pack_kernel,
        out_shape=(cells, cells, jax.ShapeDtypeStruct((MEMBERS, 1, SLOTS), jnp.int32)),
        in_specs=[HBM] * 6,
        out_specs=(VMEM, VMEM, VMEM),
        scratch_shapes=[loose, loose]
        + [pltpu.VMEM((CL, CELLS), f32)] * 2
        + [pltpu.VMEM((1, SLOTS), jnp.int32)] * 2
        + [pltpu.SemaphoreType.DMA((6,))],
        compiler_params=pltpu.CompilerParams(vmem_limit_bytes=4 * 2**20),
        name="pack",
    )(
        *(
            pltpu.with_memory_space_constraint(value, pltpu.HBM)
            for value in (
                jnp.transpose(target_coords, (1, 0, 2)),
                target_prior,
                jnp.transpose(source_coords, (1, 0, 2)),
                source_logmass,
                pair_source.reshape(1, SLOTS),
                pair_target.reshape(1, SLOTS),
            )
        )
    )
    t2 = fetched(t, lambda x, y, z, c: (x, y, z + x + FAR, c))
    t0 = fetched(t, lambda x, y, z, c: (x, y, z + x, c))
    s1, s2, s3 = (from_y(s0, k) for k in (1, 2, 3))
    codes = exchanged(codes, PLANES).reshape(MEMBERS, SLOTS)
    t1, t3 = from_core(t0), from_core(t2)
    shards = (s0, s1, s2, s3, t0, t1, t2, t3)

    shared = (
        [pltpu.VMEM((4 * CL + 1, 8, CELLS), f32)] * 2
        + [pltpu.VMEM((CELLS, CELLS), f32)] * DEEP
        + [pltpu.VMEM((8, CELLS), f32)] * DEEP
        + [pltpu.SemaphoreType.DMA((2,))]
    )
    params = pltpu.CompilerParams(vmem_limit_bytes=16 * 2**20)
    rows, pairs, xn, yn, mass, square = pl.pallas_call(
        row_kernel,
        out_shape=(
            jax.ShapeDtypeStruct((MEMBERS, 4, CL, CELLS), f32),
            jax.ShapeDtypeStruct((LIST,), jnp.int32),
            jax.ShapeDtypeStruct((4 * CL + 1, DEPTH, CELLS), bf16),
            jax.ShapeDtypeStruct((4 * CL, DEPTH, CELLS), bf16),
            jax.ShapeDtypeStruct((4 * CL, CELLS), f32),
            jax.ShapeDtypeStruct((4 * CL, CELLS), f32),
        ),
        in_specs=[ANY] + [VMEM] * 8,
        out_specs=(VMEM, ANY, VMEM, VMEM, VMEM, VMEM),
        scratch_shapes=[
            pltpu.SMEM((MEMBERS, SLOTS), jnp.int32),
            pltpu.SMEM((LIST,), jnp.int32),
            pltpu.VMEM((4 * CL, CELLS, DEPTH), bf16),
        ]
        + shared,
        compiler_params=params,
        name="rows",
    )(codes, *shards)

    rows = exchanged(rows, PLANES)

    kept, given, source_potential = pl.pallas_call(
        column_kernel,
        out_shape=(
            jax.ShapeDtypeStruct((2 * CL, CELLS), f32),
            jax.ShapeDtypeStruct((2 * CL, CELLS), f32),
            jax.ShapeDtypeStruct((CL, CELLS), f32),
        ),
        in_specs=[ANY] + [VMEM] * 5,
        out_specs=(VMEM, VMEM, VMEM),
        scratch_shapes=[
            pltpu.SMEM((LIST,), jnp.int32),
            pltpu.VMEM((DEPTH, CELLS), bf16),
            pltpu.VMEM((4 * CL + 1, CELLS, DEPTH), bf16),
            pltpu.VMEM((4, CL, CELLS), f32),
        ]
        + shared,
        compiler_params=params,
        name="columns",
    )(pairs, rows, mass, square, xn, yn)

    kept = merged([kept, from_core(given)])
    first = fetched(kept[:CL], lambda x, y, z, c: (x, y, z - x, c))
    second = fetched(kept[CL:], lambda x, y, z, c: (x, y, z - x - FAR, c))
    part = merged([first, second])
    opposite = from_x(part, 2)
    part = merged([part, opposite] + [from_x(part, k) for k in (1, 3)])
    target_potential = EPSILON * target_logmass + target_prior - (EPSILON * LN2) * part
    return source_potential, target_potential


def solution(mesh):
    return jax.shard_map(
        work,
        mesh=mesh,
        in_specs=(
            P("own", None, None),
            P("own", None, None),
            P("own", None),
            P("own", None),
            P("own", None),
            P("own", "split", None, None),
            P("own", "split", None, None),
        ),
        out_specs=(P("own", None), P("own", None)),
        check_vma=False,
    )
```

```python
import math

import jax
import jax.numpy as jnp
from jax import lax
from jax.experimental import pallas as pl
from jax.experimental.pallas import tpu as pltpu
from jax.sharding import PartitionSpec as P


EPSILON = 0.5
NEGATIVE = -1e30
LN2 = math.log(2.0)
SCALE = 1.0 / (EPSILON * LN2)

COMP = 50
CL = 4
CELLS = 256
PACKED = 56
NY, NZ, NC, NX = 4, 8, 2, 4
AXES = ("own", "split")

FAR = NZ // 2

BLOCK = 64
DEPTH = 2 * BLOCK
SLOTS = 64
DEEP = 4
LIST = SLOTS + 16

f32, bf16 = jnp.float32, jnp.bfloat16


def device(x, y, z, c):
    return (((y % NY) * NZ + z % NZ) * NC + c % NC) * NX + x % NX


def fetched(value, source):
    pairs = [
        (device(*source(x, y, z, c)), device(x, y, z, c))
        for y in range(NY)
        for z in range(NZ)
        for c in range(NC)
        for x in range(NX)
    ]
    return lax.ppermute(value, AXES, pairs)


def from_x(value, k):
    return fetched(value, lambda x, y, z, c: (x + k, y, z, c))


def from_y(value, k):
    return fetched(value, lambda x, y, z, c: (x, y + k, z, c))


PLANES = [[device(x, y, z, c) for x in range(NX) for y in range(NY)] for z in range(NZ) for c in range(NC)]
MEMBERS = 16


def exchanged(value, groups):
    return lax.all_to_all(value, AXES, 0, 0, axis_index_groups=groups, tiled=True)


def from_core(value):
    return fetched(value, lambda x, y, z, c: (x, y, z, c + 1))


def three_parts(v):
    high = v.astype(bf16).astype(f32)
    rest = v - high
    middle = rest.astype(bf16).astype(f32)
    return high, middle, rest - middle


def place():
    own, x = lax.axis_index("own"), lax.axis_index("split")
    return x, own // (NZ * NC), (own // NC) % NZ, own % NC


def target_owners():
    x, y, z, c = place()
    row = y * (NZ * NC)
    near = row + ((z + x) % NZ) * NC
    far = row + ((z + x + NZ // 2) % NZ) * NC
    return near + c, near + 1 - c, far + c, far + 1 - c


def centre(ref):
    middle = jnp.mean(ref[0:56, :], axis=1, keepdims=True)
    return jnp.broadcast_to(middle, (56, CELLS))


def load_cluster(ref, a, middle):
    at = PACKED * a
    top = ref[at : at + 48, :] - middle[0:48]
    tail = ref[at + 48 : at + PACKED, :]
    row = lax.broadcasted_iota(jnp.int32, (8, CELLS), 0)
    extra = tail[2:3, :]
    tail = jnp.where(row < 2, tail - middle[48:56], 0.0)
    square = jnp.sum(top * top, axis=0, keepdims=True) + jnp.sum(tail * tail, axis=0, keepdims=True)
    return top, tail, extra, square


def with_rows(tail, first, second):
    row = lax.broadcasted_iota(jnp.int32, (8, CELLS), 0)
    for k in range(3):
        tail = jnp.where(row == 2 + k, first[k], tail)
        tail = jnp.where(row == 5 + k, second[k], tail)
    return tail


def store_operand(ref, n, top, tail, first, second):
    zeros = jnp.zeros((8, CELLS), f32)
    for part, (head, end) in enumerate(zip(three_parts(top)[:2], three_parts(tail)[:2])):
        end = with_rows(end, first, second) if part == 0 else end
        at = part * BLOCK
        ref[n, at : at + 48, :] = head.astype(bf16)
        ref[n, at + 48 : at + BLOCK, :] = jnp.concatenate([end, zeros], axis=0).astype(bf16)


def logsum(top, total):
    return jnp.where(total > 0.0, top + jnp.log2(total), NEGATIVE)


def merged(parts):
    top = parts[0]
    for part in parts[1:]:
        top = jnp.maximum(top, part)
    total = sum(jnp.exp2(part - top) for part in parts)
    return top + jnp.log2(total)


def over_pairs(count, list_ref, left_ref, right_ref, pick, top_ref, sum_ref, scores, tops):
    def multiply(n, k):
        pair = list_ref[n]
        left, right, _ = pick(pair >> 8, pair & 255)
        cells = left_ref[left]
        high, low = right_ref[right, 0:BLOCK, :], right_ref[right, BLOCK:DEPTH, :]
        e = jnp.dot(
            jnp.concatenate([cells, cells], axis=1),
            jnp.concatenate([high, high, low, low], axis=0),
            preferred_element_type=f32,
        )
        scores[k][...] = e
        tops[k][...] = jnp.max(e.reshape(CELLS // 8, 8, CELLS), axis=0)

    def absorb(n, k):
        pair = list_ref[n]
        _, _, place = pick(pair >> 8, pair & 255)
        top = tops[k][...]
        e = scores[k][...].reshape(CELLS // 8, 8, CELLS)
        total = jnp.sum(jnp.exp2(e - top[None]), axis=0)
        old = top_ref[place]
        new = jnp.maximum(old, top)
        sum_ref[place] = sum_ref[place] * jnp.exp2(old - new) + total * jnp.exp2(top - new)
        top_ref[place] = new

    def step(q, carry):
        absorb(4 * q + 0, 0)
        multiply(4 * q + 4, 0)
        absorb(4 * q + 1, 1)
        multiply(4 * q + 5, 1)
        absorb(4 * q + 2, 2)
        multiply(4 * q + 6, 2)
        absorb(4 * q + 3, 3)
        multiply(4 * q + 7, 3)
        return carry

    multiply(0, 0)
    multiply(1, 1)
    multiply(2, 2)
    multiply(3, 3)
    lax.fori_loop(0, (count + 3) // 4, step, 0)


def finish(top_ref, sum_ref):
    tops, sums = top_ref[0 : 4 * CL], sum_ref[0 : 4 * CL]
    top = jnp.max(tops, axis=1, keepdims=True)
    total = jnp.sum(sums * jnp.exp2(tops - top), axis=1)
    return logsum(top[:, 0, :], total)


def pack_kernel(cells_in, extra_in, more_cells_in, more_extra_in, source_in, target_in, out, more_out, codes_out, cells, more_cells, extra, more_extra, source, target, sem):
    copies = [
        pltpu.make_async_copy(a, b, sem.at[k])
        for k, (a, b) in enumerate(
            (
                (cells_in, cells),
                (extra_in, extra),
                (more_cells_in, more_cells),
                (more_extra_in, more_extra),
                (source_in, source),
                (target_in, target),
            )
        )
    ]
    for copy in (*copies[4:], *copies[:4]):
        copy.start()
    for k, (a, b, o) in enumerate(((cells, extra, out), (more_cells, more_extra, more_out))):
        copies[2 * k].wait()
        copies[2 * k + 1].wait()
        for n in range(CL):
            at = PACKED * n
            o[at : at + COMP, :] = a[:, n, :]
            o[at + COMP : at + COMP + 1, :] = b[n : n + 1, :]
            o[at + COMP + 1 : at + PACKED, :] = jnp.zeros((PACKED - COMP - 1, CELLS), f32)
    copies[4].wait()
    copies[5].wait()
    codes = jnp.where(target[...] >= 0, source[...] * CL + target[...], -1)
    codes_out[...] = jnp.broadcast_to(codes[None], codes_out.shape)


def row_kernel(codes_in, s0, s1, s2, s3, t0, t1, t2, t3, out, list_out, xn, yn, mass, square_out, codes, list_ref, yt, top, tot, *rest):
    scores, tops, sem = rest[:DEEP], rest[DEEP : 2 * DEEP], rest[2 * DEEP]
    arriving = pltpu.make_async_copy(codes_in, codes, sem.at[0])
    arriving.start()
    one = jnp.ones((1, CELLS), f32)
    ones = (one, one, one)
    middle = centre(s0)
    for k, ref in enumerate((s0, s1, s2, s3)):
        for a in range(CL):
            head, tail, extra, square = load_cluster(ref, a, middle)
            mass[k * CL + a : k * CL + a + 1, :] = extra
            square_out[k * CL + a : k * CL + a + 1, :] = square
            weight = three_parts(-square * SCALE)
            store_operand(xn, k * CL + a, head * (2.0 * SCALE), tail * (2.0 * SCALE), weight, ones)
    top[...] = jnp.full(top.shape, NEGATIVE, f32)
    tot[...] = jnp.zeros(tot.shape, f32)
    arriving.wait()
    owners = target_owners()
    count = jnp.int32(0)
    y = place()[1]
    for k in range(4):
        for d in range(NX):
            for t in range(4):
                code = codes[d * NY + (y + k) % NY, owners[t]]
                source = k * CL + (code >> 2)
                list_ref[count] = source * 256 + t * CL + (code & 3)
                count = count + (code >= 0).astype(jnp.int32)
    for k in range(2 * DEEP):
        list_ref[count + k] = 4 * CL * 256
    list_ref[LIST - 1] = count
    leaving = pltpu.make_async_copy(list_ref, list_out, sem.at[1])
    leaving.start()
    xn[4 * CL] = jnp.zeros((DEPTH, CELLS), bf16)
    for k, ref in enumerate((t0, t1, t2, t3)):
        for a in range(CL):
            head, tail, prior, square = load_cluster(ref, a, middle)
            weight = three_parts((prior - square) * SCALE)
            store_operand(yn, k * CL + a, head, tail, ones, weight)
            yt[k * CL + a] = yn[k * CL + a].T
    over_pairs(count, list_ref, yt, xn, lambda s, t: (t, s, s), top, tot, scores, tops)
    rows = finish(top, tot).reshape(4, CL, CELLS)
    for k in range(4):
        for m in range(MEMBERS):
            out[m, (y + k) % NY] = rows[k]
    leaving.wait()


def column_kernel(list_in, came, mass, square, x_in, yn, kept, given, own, list_ref, xn, xt, four, top, tot, *rest):
    scores, tops, sem = rest[:DEEP], rest[DEEP : 2 * DEEP], rest[2 * DEEP]
    arriving = pltpu.make_async_copy(list_in, list_ref, sem.at[0])
    arriving.start()
    y = place()[1]
    four[...] = merged([came[m] for m in range(MEMBERS)])
    row = lax.broadcasted_iota(jnp.int32, (16, CELLS), 0)
    for k in range(4):
        rows = four[(y + k) % NY]
        if k == 0:
            own[...] = rows
        for a in range(CL):
            n = k * CL + a
            p = EPSILON * mass[n : n + 1, :] - (EPSILON * LN2) * rows[a : a + 1]
            weight = three_parts((p - square[n : n + 1, :]) * SCALE)
            xn[...] = x_in[n]
            end = xn[48:64, :].astype(f32)
            for part in range(3):
                end = jnp.where(row == 2 + part, weight[part], end)
            xn[48:64, :] = end.astype(bf16)
            xt[n] = xn[...].T
    xt[4 * CL] = jnp.zeros((CELLS, DEPTH), bf16)
    top[...] = jnp.full(top.shape, NEGATIVE, f32)
    tot[...] = jnp.zeros(tot.shape, f32)
    arriving.wait()

    def pick(s, t):
        return s, t, jnp.where(s == 4 * CL, 4 * CL, t)

    over_pairs(list_ref[LIST - 1], list_ref, xt, yn, pick, top, tot, scores, tops)
    columns = finish(top, tot)
    for k in range(2):
        kept[k * CL : (k + 1) * CL, :] = columns[2 * k * CL : (2 * k + 1) * CL]
        given[k * CL : (k + 1) * CL, :] = columns[(2 * k + 1) * CL : (2 * k + 2) * CL]


VMEM = pl.BlockSpec(memory_space=pltpu.VMEM)
ANY = pl.BlockSpec(memory_space=pl.ANY)
HBM = pl.BlockSpec(memory_space=pltpu.HBM)


def work(source_coords, target_coords, source_logmass, target_logmass, target_prior, pair_source, pair_target):
    cells = jax.ShapeDtypeStruct((CL * PACKED, CELLS), f32)
    loose = pltpu.VMEM((COMP, CL, CELLS), f32)
    t, s0, codes = pl.pallas_call(
        pack_kernel,
        out_shape=(cells, cells, jax.ShapeDtypeStruct((MEMBERS, 1, SLOTS), jnp.int32)),
        in_specs=[HBM] * 6,
        out_specs=(VMEM, VMEM, VMEM),
        scratch_shapes=[loose, loose]
        + [pltpu.VMEM((CL, CELLS), f32)] * 2
        + [pltpu.VMEM((1, SLOTS), jnp.int32)] * 2
        + [pltpu.SemaphoreType.DMA((6,))],
        compiler_params=pltpu.CompilerParams(vmem_limit_bytes=4 * 2**20),
        name="pack",
    )(
        *(
            pltpu.with_memory_space_constraint(value, pltpu.HBM)
            for value in (
                jnp.transpose(target_coords, (1, 0, 2)),
                target_prior,
                jnp.transpose(source_coords, (1, 0, 2)),
                source_logmass,
                pair_source.reshape(1, SLOTS),
                pair_target.reshape(1, SLOTS),
            )
        )
    )
    t2 = fetched(t, lambda x, y, z, c: (x, y, z + x + FAR, c))
    t0 = fetched(t, lambda x, y, z, c: (x, y, z + x, c))
    s1, s2, s3 = (from_y(s0, k) for k in (1, 2, 3))
    codes = exchanged(codes, PLANES).reshape(MEMBERS, SLOTS)
    t1, t3 = from_core(t0), from_core(t2)
    shards = (s0, s1, s2, s3, t0, t1, t2, t3)

    shared = (
        [pltpu.VMEM((4 * CL + 1, 8, CELLS), f32)] * 2
        + [pltpu.VMEM((CELLS, CELLS), f32)] * DEEP
        + [pltpu.VMEM((8, CELLS), f32)] * DEEP
        + [pltpu.SemaphoreType.DMA((2,))]
    )
    params = pltpu.CompilerParams(vmem_limit_bytes=16 * 2**20)
    rows, pairs, xn, yn, mass, square = pl.pallas_call(
        row_kernel,
        out_shape=(
            jax.ShapeDtypeStruct((MEMBERS, 4, CL, CELLS), f32),
            jax.ShapeDtypeStruct((LIST,), jnp.int32),
            jax.ShapeDtypeStruct((4 * CL + 1, DEPTH, CELLS), bf16),
            jax.ShapeDtypeStruct((4 * CL, DEPTH, CELLS), bf16),
            jax.ShapeDtypeStruct((4 * CL, CELLS), f32),
            jax.ShapeDtypeStruct((4 * CL, CELLS), f32),
        ),
        in_specs=[ANY] + [VMEM] * 8,
        out_specs=(VMEM, ANY, VMEM, VMEM, VMEM, VMEM),
        scratch_shapes=[
            pltpu.SMEM((MEMBERS, SLOTS), jnp.int32),
            pltpu.SMEM((LIST,), jnp.int32),
            pltpu.VMEM((4 * CL, CELLS, DEPTH), bf16),
        ]
        + shared,
        compiler_params=params,
        name="rows",
    )(codes, *shards)

    rows = exchanged(rows, PLANES)

    kept, given, own = pl.pallas_call(
        column_kernel,
        out_shape=(
            jax.ShapeDtypeStruct((2 * CL, CELLS), f32),
            jax.ShapeDtypeStruct((2 * CL, CELLS), f32),
            jax.ShapeDtypeStruct((CL, CELLS), f32),
        ),
        in_specs=[ANY] + [VMEM] * 5,
        out_specs=(VMEM, VMEM, VMEM),
        scratch_shapes=[
            pltpu.SMEM((LIST,), jnp.int32),
            pltpu.VMEM((DEPTH, CELLS), bf16),
            pltpu.VMEM((4 * CL + 1, CELLS, DEPTH), bf16),
            pltpu.VMEM((4, CL, CELLS), f32),
        ]
        + shared,
        compiler_params=params,
        name="columns",
    )(pairs, rows, mass, square, xn, yn)

    kept = merged([kept, from_core(given)])
    first = fetched(kept[:CL], lambda x, y, z, c: (x, y, z - x, c))
    second = fetched(kept[CL:], lambda x, y, z, c: (x, y, z - x - FAR, c))
    part = merged([first, second])
    opposite = from_x(part, 2)
    part = merged([part, opposite] + [from_x(part, k) for k in (1, 3)])
    target_potential = EPSILON * target_logmass + target_prior - (EPSILON * LN2) * part
    source_potential = EPSILON * source_logmass - (EPSILON * LN2) * own
    return source_potential, target_potential


def solution(mesh):
    return jax.shard_map(
        work,
        mesh=mesh,
        in_specs=(
            P("own", None, None),
            P("own", None, None),
            P("own", None),
            P("own", None),
            P("own", None),
            P("own", "split", None, None),
            P("own", "split", None, None),
        ),
        out_specs=(P("own", None), P("own", None)),
        check_vma=False,
    )
```

```python
import math

import jax
import jax.numpy as jnp
from jax import lax
from jax.experimental import pallas as pl
from jax.experimental.pallas import tpu as pltpu
from jax.sharding import PartitionSpec as P


EPSILON = 0.5
NEGATIVE = -1e30
LN2 = math.log(2.0)
SCALE = 1.0 / (EPSILON * LN2)

COMP = 50
CL = 4
CELLS = 256
PACKED = 56
NY, NZ, NC, NX = 4, 8, 2, 4
AXES = ("own", "split")

FAR = NZ // 2

BLOCK = 64
DEPTH = 2 * BLOCK
SLOTS = 64
DEEP = 4
LIST = SLOTS + 16

f32, bf16 = jnp.float32, jnp.bfloat16


def device(x, y, z, c):
    return (((y % NY) * NZ + z % NZ) * NC + c % NC) * NX + x % NX


def fetched(value, source):
    pairs = [
        (device(*source(x, y, z, c)), device(x, y, z, c))
        for y in range(NY)
        for z in range(NZ)
        for c in range(NC)
        for x in range(NX)
    ]
    return lax.ppermute(value, AXES, pairs)


def from_x(value, k):
    return fetched(value, lambda x, y, z, c: (x + k, y, z, c))


def from_y(value, k):
    return fetched(value, lambda x, y, z, c: (x, y + k, z, c))


PLANES = [[device(x, y, z, c) for x in range(NX) for y in range(NY)] for z in range(NZ) for c in range(NC)]
MEMBERS = 16


def exchanged(value, groups):
    return lax.all_to_all(value, AXES, 0, 0, axis_index_groups=groups, tiled=True)


def from_core(value):
    return fetched(value, lambda x, y, z, c: (x, y, z, c + 1))


def three_parts(v):
    high = v.astype(bf16).astype(f32)
    rest = v - high
    middle = rest.astype(bf16).astype(f32)
    return high, middle, rest - middle


def place():
    own, x = lax.axis_index("own"), lax.axis_index("split")
    return x, own // (NZ * NC), (own // NC) % NZ, own % NC


def target_owners():
    x, y, z, c = place()
    row = y * (NZ * NC)
    near = row + ((z + x) % NZ) * NC
    far = row + ((z + x + NZ // 2) % NZ) * NC
    return near + c, near + 1 - c, far + c, far + 1 - c


def centre(ref):
    middle = jnp.mean(ref[0], axis=1, keepdims=True)
    return jnp.broadcast_to(middle, (PACKED, CELLS))


def load_cluster(ref, a, middle):
    top = ref[a, 0:48, :] - middle[0:48]
    tail = ref[a, 48:PACKED, :]
    row = lax.broadcasted_iota(jnp.int32, (8, CELLS), 0)
    extra = tail[2:3, :]
    tail = jnp.where(row < 2, tail - middle[48:56], 0.0)
    square = jnp.sum(top * top, axis=0, keepdims=True) + jnp.sum(tail * tail, axis=0, keepdims=True)
    return top, tail, extra, square


def with_rows(tail, first, second):
    row = lax.broadcasted_iota(jnp.int32, (8, CELLS), 0)
    for k in range(3):
        tail = jnp.where(row == 2 + k, first[k], tail)
        tail = jnp.where(row == 5 + k, second[k], tail)
    return tail


def store_operand(ref, n, top, tail, first, second):
    zeros = jnp.zeros((8, CELLS), f32)
    for part, (head, end) in enumerate(zip(three_parts(top)[:2], three_parts(tail)[:2])):
        end = with_rows(end, first, second) if part == 0 else end
        at = part * BLOCK
        ref[n, at : at + 48, :] = head.astype(bf16)
        ref[n, at + 48 : at + BLOCK, :] = jnp.concatenate([end, zeros], axis=0).astype(bf16)


def logsum(top, total):
    return jnp.where(total > 0.0, top + jnp.log2(total), NEGATIVE)


def merged(parts):
    top = parts[0]
    for part in parts[1:]:
        top = jnp.maximum(top, part)
    total = sum(jnp.exp2(part - top) for part in parts)
    return top + jnp.log2(total)


def over_pairs(count, list_ref, left_ref, right_ref, pick, top_ref, sum_ref, scores, tops):
    def multiply(n, k):
        pair = list_ref[n]
        left, right, _ = pick(pair >> 8, pair & 255)
        cells = left_ref[left]
        high, low = right_ref[right, 0:BLOCK, :], right_ref[right, BLOCK:DEPTH, :]
        e = jnp.dot(
            jnp.concatenate([cells, cells], axis=1),
            jnp.concatenate([high, high, low, low], axis=0),
            preferred_element_type=f32,
        )
        scores[k][...] = e
        tops[k][...] = jnp.max(e.reshape(CELLS // 8, 8, CELLS), axis=0)

    def absorb(n, k):
        pair = list_ref[n]
        _, _, place = pick(pair >> 8, pair & 255)
        top = tops[k][...]
        e = scores[k][...].reshape(CELLS // 8, 8, CELLS)
        total = jnp.sum(jnp.exp2(e - top[None]), axis=0)
        old = top_ref[place]
        new = jnp.maximum(old, top)
        sum_ref[place] = sum_ref[place] * jnp.exp2(old - new) + total * jnp.exp2(top - new)
        top_ref[place] = new

    def step(q, carry):
        absorb(4 * q + 0, 0)
        multiply(4 * q + 4, 0)
        absorb(4 * q + 1, 1)
        multiply(4 * q + 5, 1)
        absorb(4 * q + 2, 2)
        multiply(4 * q + 6, 2)
        absorb(4 * q + 3, 3)
        multiply(4 * q + 7, 3)
        return carry

    multiply(0, 0)
    multiply(1, 1)
    multiply(2, 2)
    multiply(3, 3)
    lax.fori_loop(0, (count + 3) // 4, step, 0)


def finish(top_ref, sum_ref):
    tops, sums = top_ref[0 : 4 * CL], sum_ref[0 : 4 * CL]
    top = jnp.max(tops, axis=1, keepdims=True)
    total = jnp.sum(sums * jnp.exp2(tops - top), axis=1)
    return logsum(top[:, 0, :], total)


def pack_kernel(cells_in, extra_in, more_cells_in, more_extra_in, out, more_out, cells, more_cells, extra, more_extra, sem):
    copies = [
        pltpu.make_async_copy(a, b, sem.at[k])
        for k, (a, b) in enumerate(
            (
                (cells_in, cells),
                (extra_in, extra),
                (more_cells_in, more_cells),
                (more_extra_in, more_extra),
            )
        )
    ]
    for copy in copies:
        copy.start()
    for k, (a, b, o) in enumerate(((cells, extra, out), (more_cells, more_extra, more_out))):
        copies[2 * k].wait()
        copies[2 * k + 1].wait()
        for n in range(CL):
            o[n, 0:COMP, :] = a[:, n, :]
            o[n, COMP : COMP + 1, :] = b[n : n + 1, :]
            o[n, COMP + 1 : PACKED, :] = jnp.zeros((PACKED - COMP - 1, CELLS), f32)


def row_kernel(codes_in, s0, s1, s2, s3, t0, t1, t2, t3, out, list_out, xn, yn, mass, square_out, codes, list_ref, yt, top, tot, *rest):
    scores, tops, sem = rest[:DEEP], rest[DEEP : 2 * DEEP], rest[2 * DEEP]
    arriving = pltpu.make_async_copy(codes_in, codes, sem.at[0])
    arriving.start()
    one = jnp.ones((1, CELLS), f32)
    ones = (one, one, one)
    middle = centre(s0)
    for k, ref in enumerate((s0, s1, s2, s3)):
        for a in range(CL):
            head, tail, extra, square = load_cluster(ref, a, middle)
            mass[k * CL + a : k * CL + a + 1, :] = extra
            square_out[k * CL + a : k * CL + a + 1, :] = square
            weight = three_parts(-square * SCALE)
            store_operand(xn, k * CL + a, head * (2.0 * SCALE), tail * (2.0 * SCALE), weight, ones)
    top[...] = jnp.full(top.shape, NEGATIVE, f32)
    tot[...] = jnp.zeros(tot.shape, f32)
    arriving.wait()
    owners = target_owners()
    count = jnp.int32(0)
    y = place()[1]
    for k in range(4):
        for d in range(NX):
            for t in range(4):
                code = codes[d * NY + (y + k) % NY, owners[t]]
                source = k * CL + (code >> 2)
                list_ref[count] = source * 256 + t * CL + (code & 3)
                count = count + (code >= 0).astype(jnp.int32)
    for k in range(2 * DEEP):
        list_ref[count + k] = 4 * CL * 256
    list_ref[LIST - 1] = count
    leaving = pltpu.make_async_copy(list_ref, list_out, sem.at[1])
    leaving.start()
    xn[4 * CL] = jnp.zeros((DEPTH, CELLS), bf16)
    for k, ref in enumerate((t0, t1, t2, t3)):
        for a in range(CL):
            head, tail, prior, square = load_cluster(ref, a, middle)
            weight = three_parts((prior - square) * SCALE)
            store_operand(yn, k * CL + a, head, tail, ones, weight)
            yt[k * CL + a] = yn[k * CL + a].T
    over_pairs(count, list_ref, yt, xn, lambda s, t: (t, s, s), top, tot, scores, tops)
    rows = finish(top, tot).reshape(4, CL, CELLS)
    for k in range(4):
        for m in range(MEMBERS):
            out[m, (y + k) % NY] = rows[k]
    leaving.wait()


def column_kernel(list_in, came, mass, square, x_in, yn, kept, given, own, list_ref, xn, xt, four, top, tot, *rest):
    scores, tops, sem = rest[:DEEP], rest[DEEP : 2 * DEEP], rest[2 * DEEP]
    arriving = pltpu.make_async_copy(list_in, list_ref, sem.at[0])
    arriving.start()
    y = place()[1]
    four[...] = merged([came[m] for m in range(MEMBERS)])
    row = lax.broadcasted_iota(jnp.int32, (16, CELLS), 0)
    for k in range(4):
        rows = four[(y + k) % NY]
        if k == 0:
            own[...] = rows
        for a in range(CL):
            n = k * CL + a
            p = EPSILON * mass[n : n + 1, :] - (EPSILON * LN2) * rows[a : a + 1]
            weight = three_parts((p - square[n : n + 1, :]) * SCALE)
            xn[...] = x_in[n]
            end = xn[48:64, :].astype(f32)
            for part in range(3):
                end = jnp.where(row == 2 + part, weight[part], end)
            xn[48:64, :] = end.astype(bf16)
            xt[n] = xn[...].T
    xt[4 * CL] = jnp.zeros((CELLS, DEPTH), bf16)
    top[...] = jnp.full(top.shape, NEGATIVE, f32)
    tot[...] = jnp.zeros(tot.shape, f32)
    arriving.wait()

    def pick(s, t):
        return s, t, jnp.where(s == 4 * CL, 4 * CL, t)

    over_pairs(list_ref[LIST - 1], list_ref, xt, yn, pick, top, tot, scores, tops)
    columns = finish(top, tot)
    for k in range(2):
        kept[k * CL : (k + 1) * CL, :] = columns[2 * k * CL : (2 * k + 1) * CL]
        given[k * CL : (k + 1) * CL, :] = columns[(2 * k + 1) * CL : (2 * k + 2) * CL]


VMEM = pl.BlockSpec(memory_space=pltpu.VMEM)
ANY = pl.BlockSpec(memory_space=pl.ANY)
HBM = pl.BlockSpec(memory_space=pltpu.HBM)


def work(source_coords, target_coords, source_logmass, target_logmass, target_prior, pair_source, pair_target):
    codes = pair_source * 4 + pair_target
    codes = jnp.where(pair_target >= 0, codes, -1).reshape(1, -1)
    codes = exchanged(jnp.broadcast_to(codes, (MEMBERS, codes.shape[1])), PLANES)

    cells = jax.ShapeDtypeStruct((CL, PACKED, CELLS), f32)
    loose = pltpu.VMEM((COMP, CL, CELLS), f32)
    t, s0 = pl.pallas_call(
        pack_kernel,
        out_shape=(cells, cells),
        in_specs=[HBM] * 4,
        out_specs=(VMEM, VMEM),
        scratch_shapes=[loose, loose] + [pltpu.VMEM((CL, CELLS), f32)] * 2 + [pltpu.SemaphoreType.DMA((4,))],
        compiler_params=pltpu.CompilerParams(vmem_limit_bytes=4 * 2**20),
        name="pack",
    )(
        *(
            pltpu.with_memory_space_constraint(value, pltpu.HBM)
            for value in (
                jnp.transpose(target_coords, (1, 0, 2)),
                target_prior,
                jnp.transpose(source_coords, (1, 0, 2)),
                source_logmass,
            )
        )
    )
    t2 = fetched(t, lambda x, y, z, c: (x, y, z + x + FAR, c))
    t0 = fetched(t, lambda x, y, z, c: (x, y, z + x, c))
    s1, s2, s3 = (from_y(s0, k) for k in (1, 2, 3))
    t1, t3 = from_core(t0), from_core(t2)
    shards = (s0, s1, s2, s3, t0, t1, t2, t3)

    shared = (
        [pltpu.VMEM((4 * CL + 1, 8, CELLS), f32)] * 2
        + [pltpu.VMEM((CELLS, CELLS), f32)] * DEEP
        + [pltpu.VMEM((8, CELLS), f32)] * DEEP
        + [pltpu.SemaphoreType.DMA((2,))]
    )
    params = pltpu.CompilerParams(vmem_limit_bytes=16 * 2**20)
    rows, pairs, xn, yn, mass, square = pl.pallas_call(
        row_kernel,
        out_shape=(
            jax.ShapeDtypeStruct((MEMBERS, 4, CL, CELLS), f32),
            jax.ShapeDtypeStruct((LIST,), jnp.int32),
            jax.ShapeDtypeStruct((4 * CL + 1, DEPTH, CELLS), bf16),
            jax.ShapeDtypeStruct((4 * CL, DEPTH, CELLS), bf16),
            jax.ShapeDtypeStruct((4 * CL, CELLS), f32),
            jax.ShapeDtypeStruct((4 * CL, CELLS), f32),
        ),
        in_specs=[ANY] + [VMEM] * 8,
        out_specs=(VMEM, ANY, VMEM, VMEM, VMEM, VMEM),
        scratch_shapes=[
            pltpu.SMEM((MEMBERS, SLOTS), jnp.int32),
            pltpu.SMEM((LIST,), jnp.int32),
            pltpu.VMEM((4 * CL, CELLS, DEPTH), bf16),
        ]
        + shared,
        compiler_params=params,
        name="rows",
    )(codes, *shards)

    rows = exchanged(rows, PLANES)

    kept, given, own = pl.pallas_call(
        column_kernel,
        out_shape=(
            jax.ShapeDtypeStruct((2 * CL, CELLS), f32),
            jax.ShapeDtypeStruct((2 * CL, CELLS), f32),
            jax.ShapeDtypeStruct((CL, CELLS), f32),
        ),
        in_specs=[ANY] + [VMEM] * 5,
        out_specs=(VMEM, VMEM, VMEM),
        scratch_shapes=[
            pltpu.SMEM((LIST,), jnp.int32),
            pltpu.VMEM((DEPTH, CELLS), bf16),
            pltpu.VMEM((4 * CL + 1, CELLS, DEPTH), bf16),
            pltpu.VMEM((4, CL, CELLS), f32),
        ]
        + shared,
        compiler_params=params,
        name="columns",
    )(pairs, rows, mass, square, xn, yn)

    kept = merged([kept, from_core(given)])
    first = fetched(kept[:CL], lambda x, y, z, c: (x, y, z - x, c))
    second = fetched(kept[CL:], lambda x, y, z, c: (x, y, z - x - FAR, c))
    part = merged([first, second])
    part = merged([part] + [from_x(part, k) for k in (1, 2, 3)])
    target_potential = EPSILON * target_logmass + target_prior - (EPSILON * LN2) * part
    source_potential = EPSILON * source_logmass - (EPSILON * LN2) * own
    return source_potential, target_potential


def solution(mesh):
    return jax.shard_map(
        work,
        mesh=mesh,
        in_specs=(
            P("own", None, None),
            P("own", None, None),
            P("own", None),
            P("own", None),
            P("own", None),
            P("own", "split", None, None),
            P("own", "split", None, None),
        ),
        out_specs=(P("own", None), P("own", None)),
        check_vma=False,
    )
```

```python
import math

import jax
import jax.numpy as jnp
from jax import lax
from jax.experimental import pallas as pl
from jax.experimental.pallas import tpu as pltpu
from jax.sharding import PartitionSpec as P


EPSILON = 0.5
NEGATIVE = -1e30
LN2 = math.log(2.0)
SCALE = 1.0 / (EPSILON * LN2)

COMP = 50
CL = 4
CELLS = 256
PACKED = 56
NY, NZ, NC, NX = 4, 8, 2, 4
AXES = ("own", "split")

FAR = NZ // 2

BLOCK = 64
DEPTH = 2 * BLOCK
SLOTS = 64
DEEP = 4
LIST = SLOTS + 16

f32, bf16 = jnp.float32, jnp.bfloat16


def device(x, y, z, c):
    return (((y % NY) * NZ + z % NZ) * NC + c % NC) * NX + x % NX


def fetched(value, source):
    pairs = [
        (device(*source(x, y, z, c)), device(x, y, z, c))
        for y in range(NY)
        for z in range(NZ)
        for c in range(NC)
        for x in range(NX)
    ]
    return lax.ppermute(value, AXES, pairs)


def from_x(value, k):
    return fetched(value, lambda x, y, z, c: (x + k, y, z, c))


def from_y(value, k):
    return fetched(value, lambda x, y, z, c: (x, y + k, z, c))


PLANES = [[device(x, y, z, c) for x in range(NX) for y in range(NY)] for z in range(NZ) for c in range(NC)]
MEMBERS = 16


def exchanged(value, groups):
    return lax.all_to_all(value, AXES, 0, 0, axis_index_groups=groups, tiled=True)


def from_core(value):
    return fetched(value, lambda x, y, z, c: (x, y, z, c + 1))


def three_parts(v):
    high = v.astype(bf16).astype(f32)
    rest = v - high
    middle = rest.astype(bf16).astype(f32)
    return high, middle, rest - middle


def place():
    own, x = lax.axis_index("own"), lax.axis_index("split")
    return x, own // (NZ * NC), (own // NC) % NZ, own % NC


def target_owners():
    x, y, z, c = place()
    row = y * (NZ * NC)
    near = row + ((z + x) % NZ) * NC
    far = row + ((z + x + NZ // 2) % NZ) * NC
    return near + c, near + 1 - c, far + c, far + 1 - c


def centre(ref):
    middle = jnp.mean(ref[0], axis=1, keepdims=True)
    return jnp.broadcast_to(middle, (PACKED, CELLS))


def load_cluster(ref, a, middle):
    top = ref[a, 0:48, :] - middle[0:48]
    tail = ref[a, 48:PACKED, :]
    row = lax.broadcasted_iota(jnp.int32, (8, CELLS), 0)
    extra = tail[2:3, :]
    tail = jnp.where(row < 2, tail - middle[48:56], 0.0)
    square = jnp.sum(top * top, axis=0, keepdims=True) + jnp.sum(tail * tail, axis=0, keepdims=True)
    return top, tail, extra, square


def with_rows(tail, first, second):
    row = lax.broadcasted_iota(jnp.int32, (8, CELLS), 0)
    for k in range(3):
        tail = jnp.where(row == 2 + k, first[k], tail)
        tail = jnp.where(row == 5 + k, second[k], tail)
    return tail


def store_operand(ref, n, top, tail, first, second):
    zeros = jnp.zeros((8, CELLS), f32)
    for part, (head, end) in enumerate(zip(three_parts(top)[:2], three_parts(tail)[:2])):
        end = with_rows(end, first, second) if part == 0 else end
        at = part * BLOCK
        ref[n, at : at + 48, :] = head.astype(bf16)
        ref[n, at + 48 : at + BLOCK, :] = jnp.concatenate([end, zeros], axis=0).astype(bf16)


def logsum(top, total):
    return jnp.where(total > 0.0, top + jnp.log2(total), NEGATIVE)


def merged(parts):
    top = parts[0]
    for part in parts[1:]:
        top = jnp.maximum(top, part)
    total = sum(jnp.exp2(part - top) for part in parts)
    return top + jnp.log2(total)


def over_pairs(count, list_ref, left_ref, right_ref, pick, top_ref, sum_ref, scores, tops):
    def multiply(n, k):
        pair = list_ref[n]
        left, right, _ = pick(pair >> 8, pair & 255)
        cells = left_ref[left]
        high, low = right_ref[right, 0:BLOCK, :], right_ref[right, BLOCK:DEPTH, :]
        e = jnp.dot(
            jnp.concatenate([cells, cells], axis=1),
            jnp.concatenate([high, high, low, low], axis=0),
            preferred_element_type=f32,
        )
        scores[k][...] = e
        tops[k][...] = jnp.max(e.reshape(CELLS // 8, 8, CELLS), axis=0)

    def absorb(n, k):
        pair = list_ref[n]
        _, _, place = pick(pair >> 8, pair & 255)
        top = tops[k][...]
        e = scores[k][...].reshape(CELLS // 8, 8, CELLS)
        total = jnp.sum(jnp.exp2(e - top[None]), axis=0)
        old = top_ref[place]
        new = jnp.maximum(old, top)
        sum_ref[place] = sum_ref[place] * jnp.exp2(old - new) + total * jnp.exp2(top - new)
        top_ref[place] = new

    def step(q, carry):
        absorb(4 * q + 0, 0)
        multiply(4 * q + 4, 0)
        absorb(4 * q + 1, 1)
        multiply(4 * q + 5, 1)
        absorb(4 * q + 2, 2)
        multiply(4 * q + 6, 2)
        absorb(4 * q + 3, 3)
        multiply(4 * q + 7, 3)
        return carry

    multiply(0, 0)
    multiply(1, 1)
    multiply(2, 2)
    multiply(3, 3)
    lax.fori_loop(0, (count + 3) // 4, step, 0)


def finish(top_ref, sum_ref):
    tops, sums = top_ref[0 : 4 * CL], sum_ref[0 : 4 * CL]
    top = jnp.max(tops, axis=1, keepdims=True)
    total = jnp.sum(sums * jnp.exp2(tops - top), axis=1)
    return logsum(top[:, 0, :], total)


def pack_kernel(cells_in, extra_in, more_cells_in, more_extra_in, source_in, target_in, out, more_out, codes_out, cells, more_cells, extra, more_extra, source, target, sem):
    copies = [
        pltpu.make_async_copy(a, b, sem.at[k])
        for k, (a, b) in enumerate(
            (
                (cells_in, cells),
                (extra_in, extra),
                (more_cells_in, more_cells),
                (more_extra_in, more_extra),
                (source_in, source),
                (target_in, target),
            )
        )
    ]
    for copy in copies:
        copy.start()
    for k, (a, b, o) in enumerate(((cells, extra, out), (more_cells, more_extra, more_out))):
        copies[2 * k].wait()
        copies[2 * k + 1].wait()
        for n in range(CL):
            o[n, 0:COMP, :] = a[:, n, :]
            o[n, COMP : COMP + 1, :] = b[n : n + 1, :]
            o[n, COMP + 1 : PACKED, :] = jnp.zeros((PACKED - COMP - 1, CELLS), f32)
    copies[4].wait()
    copies[5].wait()
    codes_out[...] = jnp.where(target[...] >= 0, source[...] * CL + target[...], -1)


def row_kernel(codes_in, s0, s1, s2, s3, t0, t1, t2, t3, out, list_out, xn, yn, mass, square_out, codes, list_ref, yt, top, tot, *rest):
    scores, tops, sem = rest[:DEEP], rest[DEEP : 2 * DEEP], rest[2 * DEEP]
    arriving = pltpu.make_async_copy(codes_in, codes, sem.at[0])
    arriving.start()
    one = jnp.ones((1, CELLS), f32)
    ones = (one, one, one)
    middle = centre(s0)
    for k, ref in enumerate((s0, s1, s2, s3)):
        for a in range(CL):
            head, tail, extra, square = load_cluster(ref, a, middle)
            mass[k * CL + a : k * CL + a + 1, :] = extra
            square_out[k * CL + a : k * CL + a + 1, :] = square
            weight = three_parts(-square * SCALE)
            store_operand(xn, k * CL + a, head * (2.0 * SCALE), tail * (2.0 * SCALE), weight, ones)
    top[...] = jnp.full(top.shape, NEGATIVE, f32)
    tot[...] = jnp.zeros(tot.shape, f32)
    arriving.wait()
    owners = target_owners()
    count = jnp.int32(0)
    y = place()[1]
    for k in range(4):
        for d in range(NX):
            for t in range(4):
                code = codes[d * NY + (y + k) % NY, owners[t]]
                source = k * CL + (code >> 2)
                list_ref[count] = source * 256 + t * CL + (code & 3)
                count = count + (code >= 0).astype(jnp.int32)
    for k in range(2 * DEEP):
        list_ref[count + k] = 4 * CL * 256
    list_ref[LIST - 1] = count
    leaving = pltpu.make_async_copy(list_ref, list_out, sem.at[1])
    leaving.start()
    xn[4 * CL] = jnp.zeros((DEPTH, CELLS), bf16)
    for k, ref in enumerate((t0, t1, t2, t3)):
        for a in range(CL):
            head, tail, prior, square = load_cluster(ref, a, middle)
            weight = three_parts((prior - square) * SCALE)
            store_operand(yn, k * CL + a, head, tail, ones, weight)
            yt[k * CL + a] = yn[k * CL + a].T
    over_pairs(count, list_ref, yt, xn, lambda s, t: (t, s, s), top, tot, scores, tops)
    rows = finish(top, tot).reshape(4, CL, CELLS)
    for k in range(4):
        for m in range(MEMBERS):
            out[m, (y + k) % NY] = rows[k]
    leaving.wait()


def column_kernel(list_in, came, mass, square, x_in, yn, kept, given, own, list_ref, xn, xt, four, top, tot, *rest):
    scores, tops, sem = rest[:DEEP], rest[DEEP : 2 * DEEP], rest[2 * DEEP]
    arriving = pltpu.make_async_copy(list_in, list_ref, sem.at[0])
    arriving.start()
    y = place()[1]
    four[...] = merged([came[m] for m in range(MEMBERS)])
    row = lax.broadcasted_iota(jnp.int32, (16, CELLS), 0)
    for k in range(4):
        rows = four[(y + k) % NY]
        if k == 0:
            own[...] = rows
        for a in range(CL):
            n = k * CL + a
            p = EPSILON * mass[n : n + 1, :] - (EPSILON * LN2) * rows[a : a + 1]
            weight = three_parts((p - square[n : n + 1, :]) * SCALE)
            xn[...] = x_in[n]
            end = xn[48:64, :].astype(f32)
            for part in range(3):
                end = jnp.where(row == 2 + part, weight[part], end)
            xn[48:64, :] = end.astype(bf16)
            xt[n] = xn[...].T
    xt[4 * CL] = jnp.zeros((CELLS, DEPTH), bf16)
    top[...] = jnp.full(top.shape, NEGATIVE, f32)
    tot[...] = jnp.zeros(tot.shape, f32)
    arriving.wait()

    def pick(s, t):
        return s, t, jnp.where(s == 4 * CL, 4 * CL, t)

    over_pairs(list_ref[LIST - 1], list_ref, xt, yn, pick, top, tot, scores, tops)
    columns = finish(top, tot)
    for k in range(2):
        kept[k * CL : (k + 1) * CL, :] = columns[2 * k * CL : (2 * k + 1) * CL]
        given[k * CL : (k + 1) * CL, :] = columns[(2 * k + 1) * CL : (2 * k + 2) * CL]


VMEM = pl.BlockSpec(memory_space=pltpu.VMEM)
ANY = pl.BlockSpec(memory_space=pl.ANY)
HBM = pl.BlockSpec(memory_space=pltpu.HBM)


def work(source_coords, target_coords, source_logmass, target_logmass, target_prior, pair_source, pair_target):
    cells = jax.ShapeDtypeStruct((CL, PACKED, CELLS), f32)
    loose = pltpu.VMEM((COMP, CL, CELLS), f32)
    t, s0, codes = pl.pallas_call(
        pack_kernel,
        out_shape=(cells, cells, jax.ShapeDtypeStruct((1, SLOTS), jnp.int32)),
        in_specs=[HBM] * 6,
        out_specs=(VMEM, VMEM, VMEM),
        scratch_shapes=[loose, loose] + [pltpu.VMEM((CL, CELLS), f32)] * 2
        + [pltpu.VMEM((1, SLOTS), jnp.int32)] * 2
        + [pltpu.SemaphoreType.DMA((6,))],
        compiler_params=pltpu.CompilerParams(vmem_limit_bytes=4 * 2**20),
        name="pack",
    )(
        *(
            pltpu.with_memory_space_constraint(value, pltpu.HBM)
            for value in (
                jnp.transpose(target_coords, (1, 0, 2)),
                target_prior,
                jnp.transpose(source_coords, (1, 0, 2)),
                source_logmass,
                pair_source.reshape(1, SLOTS),
                pair_target.reshape(1, SLOTS),
            )
        )
    )
    t2 = fetched(t, lambda x, y, z, c: (x, y, z + x + FAR, c))
    t0 = fetched(t, lambda x, y, z, c: (x, y, z + x, c))
    s1, s2, s3 = (from_y(s0, k) for k in (1, 2, 3))
    codes = exchanged(jnp.broadcast_to(codes, (MEMBERS, SLOTS)), PLANES)
    t1, t3 = from_core(t0), from_core(t2)
    shards = (s0, s1, s2, s3, t0, t1, t2, t3)

    shared = (
        [pltpu.VMEM((4 * CL + 1, 8, CELLS), f32)] * 2
        + [pltpu.VMEM((CELLS, CELLS), f32)] * DEEP
        + [pltpu.VMEM((8, CELLS), f32)] * DEEP
        + [pltpu.SemaphoreType.DMA((2,))]
    )
    params = pltpu.CompilerParams(vmem_limit_bytes=16 * 2**20)
    rows, pairs, xn, yn, mass, square = pl.pallas_call(
        row_kernel,
        out_shape=(
            jax.ShapeDtypeStruct((MEMBERS, 4, CL, CELLS), f32),
            jax.ShapeDtypeStruct((LIST,), jnp.int32),
            jax.ShapeDtypeStruct((4 * CL + 1, DEPTH, CELLS), bf16),
            jax.ShapeDtypeStruct((4 * CL, DEPTH, CELLS), bf16),
            jax.ShapeDtypeStruct((4 * CL, CELLS), f32),
            jax.ShapeDtypeStruct((4 * CL, CELLS), f32),
        ),
        in_specs=[ANY] + [VMEM] * 8,
        out_specs=(VMEM, ANY, VMEM, VMEM, VMEM, VMEM),
        scratch_shapes=[
            pltpu.SMEM((MEMBERS, SLOTS), jnp.int32),
            pltpu.SMEM((LIST,), jnp.int32),
            pltpu.VMEM((4 * CL, CELLS, DEPTH), bf16),
        ]
        + shared,
        compiler_params=params,
        name="rows",
    )(codes, *shards)

    rows = exchanged(rows, PLANES)

    kept, given, own = pl.pallas_call(
        column_kernel,
        out_shape=(
            jax.ShapeDtypeStruct((2 * CL, CELLS), f32),
            jax.ShapeDtypeStruct((2 * CL, CELLS), f32),
            jax.ShapeDtypeStruct((CL, CELLS), f32),
        ),
        in_specs=[ANY] + [VMEM] * 5,
        out_specs=(VMEM, VMEM, VMEM),
        scratch_shapes=[
            pltpu.SMEM((LIST,), jnp.int32),
            pltpu.VMEM((DEPTH, CELLS), bf16),
            pltpu.VMEM((4 * CL + 1, CELLS, DEPTH), bf16),
            pltpu.VMEM((4, CL, CELLS), f32),
        ]
        + shared,
        compiler_params=params,
        name="columns",
    )(pairs, rows, mass, square, xn, yn)

    kept = merged([kept, from_core(given)])
    first = fetched(kept[:CL], lambda x, y, z, c: (x, y, z - x, c))
    second = fetched(kept[CL:], lambda x, y, z, c: (x, y, z - x - FAR, c))
    part = merged([first, second])
    part = merged([part] + [from_x(part, k) for k in (1, 2, 3)])
    target_potential = EPSILON * target_logmass + target_prior - (EPSILON * LN2) * part
    source_potential = EPSILON * source_logmass - (EPSILON * LN2) * own
    return source_potential, target_potential


def solution(mesh):
    return jax.shard_map(
        work,
        mesh=mesh,
        in_specs=(
            P("own", None, None),
            P("own", None, None),
            P("own", None),
            P("own", None),
            P("own", None),
            P("own", "split", None, None),
            P("own", "split", None, None),
        ),
        out_specs=(P("own", None), P("own", None)),
        check_vma=False,
    )
```

```python
import math

import jax
import jax.numpy as jnp
from jax import lax
from jax.experimental import pallas as pl
from jax.experimental.pallas import tpu as pltpu
from jax.sharding import PartitionSpec as P


EPSILON = 0.5
NEGATIVE = -1e30
LN2 = math.log(2.0)
SCALE = 1.0 / (EPSILON * LN2)

COMP = 50
CL = 4
CELLS = 256
PACKED = 56
NY, NZ, NC, NX = 4, 8, 2, 4
AXES = ("own", "split")

NEAR = (0, 1, 2, 7)
FAR = (4, 5, 6, 3)

BLOCK = 64
DEPTH = 2 * BLOCK
SLOTS = 64
DEEP = 4
LIST = SLOTS + 16

f32, bf16 = jnp.float32, jnp.bfloat16


def device(x, y, z, c):
    return (((y % NY) * NZ + z % NZ) * NC + c % NC) * NX + x % NX


def fetched(value, source):
    pairs = [
        (device(*source(x, y, z, c)), device(x, y, z, c))
        for y in range(NY)
        for z in range(NZ)
        for c in range(NC)
        for x in range(NX)
    ]
    return lax.ppermute(value, AXES, pairs)


def from_x(value, k):
    return fetched(value, lambda x, y, z, c: (x + k, y, z, c))


def from_y(value, k):
    return fetched(value, lambda x, y, z, c: (x, y + k, z, c))


PLANES = [[device(x, y, z, c) for x in range(NX) for y in range(NY)] for z in range(NZ) for c in range(NC)]
MEMBERS = 16


def exchanged(value, groups):
    return lax.all_to_all(value, AXES, 0, 0, axis_index_groups=groups, tiled=True)


def from_core(value):
    return fetched(value, lambda x, y, z, c: (x, y, z, c + 1))


def three_parts(v):
    high = v.astype(bf16).astype(f32)
    rest = v - high
    middle = rest.astype(bf16).astype(f32)
    return high, middle, rest - middle


def place():
    own, x = lax.axis_index("own"), lax.axis_index("split")
    return x, own // (NZ * NC), (own // NC) % NZ, own % NC


def target_owners():
    x, y, z, c = place()
    row = y * (NZ * NC)
    last = (x == NX - 1).astype(jnp.int32) * (NZ // 2)
    near = row + ((z + x + last) % NZ) * NC
    far = row + ((z + x + NZ // 2 - last) % NZ) * NC
    return near + c, near + 1 - c, far + c, far + 1 - c


def centre(ref):
    middle = jnp.mean(ref[0], axis=1, keepdims=True)
    return jnp.broadcast_to(middle, (PACKED, CELLS))


def load_cluster(ref, a, middle):
    top = ref[a, 0:48, :] - middle[0:48]
    tail = ref[a, 48:PACKED, :]
    row = lax.broadcasted_iota(jnp.int32, (8, CELLS), 0)
    extra = tail[2:3, :]
    tail = jnp.where(row < 2, tail - middle[48:56], 0.0)
    square = jnp.sum(top * top, axis=0, keepdims=True) + jnp.sum(tail * tail, axis=0, keepdims=True)
    return top, tail, extra, square


def with_rows(tail, first, second):
    row = lax.broadcasted_iota(jnp.int32, (8, CELLS), 0)
    for k in range(3):
        tail = jnp.where(row == 2 + k, first[k], tail)
        tail = jnp.where(row == 5 + k, second[k], tail)
    return tail


def store_operand(ref, n, top, tail, first, second):
    zeros = jnp.zeros((8, CELLS), f32)
    for part, (head, end) in enumerate(zip(three_parts(top)[:2], three_parts(tail)[:2])):
        end = with_rows(end, first, second) if part == 0 else end
        at = part * BLOCK
        ref[n, at : at + 48, :] = head.astype(bf16)
        ref[n, at + 48 : at + BLOCK, :] = jnp.concatenate([end, zeros], axis=0).astype(bf16)


def logsum(top, total):
    return jnp.where(total > 0.0, top + jnp.log2(total), NEGATIVE)


def merged(parts):
    top = parts[0]
    for part in parts[1:]:
        top = jnp.maximum(top, part)
    total = sum(jnp.exp2(part - top) for part in parts)
    return top + jnp.log2(total)


def over_pairs(count, list_ref, left_ref, right_ref, pick, top_ref, sum_ref, scores, tops):
    def multiply(n, k):
        pair = list_ref[n]
        left, right, _ = pick(pair >> 8, pair & 255)
        cells = left_ref[left]
        high, low = right_ref[right, 0:BLOCK, :], right_ref[right, BLOCK:DEPTH, :]
        e = jnp.dot(
            jnp.concatenate([cells, cells], axis=1),
            jnp.concatenate([high, high, low, low], axis=0),
            preferred_element_type=f32,
        )
        scores[k][...] = e
        tops[k][...] = jnp.max(e.reshape(CELLS // 8, 8, CELLS), axis=0)

    def absorb(n, k):
        pair = list_ref[n]
        _, _, place = pick(pair >> 8, pair & 255)
        top = tops[k][...]
        e = scores[k][...].reshape(CELLS // 8, 8, CELLS)
        total = jnp.sum(jnp.exp2(e - top[None]), axis=0)
        old = top_ref[place]
        new = jnp.maximum(old, top)
        sum_ref[place] = sum_ref[place] * jnp.exp2(old - new) + total * jnp.exp2(top - new)
        top_ref[place] = new

    def step(q, carry):
        absorb(4 * q + 0, 0)
        multiply(4 * q + 4, 0)
        absorb(4 * q + 1, 1)
        multiply(4 * q + 5, 1)
        absorb(4 * q + 2, 2)
        multiply(4 * q + 6, 2)
        absorb(4 * q + 3, 3)
        multiply(4 * q + 7, 3)
        return carry

    multiply(0, 0)
    multiply(1, 1)
    multiply(2, 2)
    multiply(3, 3)
    lax.fori_loop(0, (count + 3) // 4, step, 0)


def finish(top_ref, sum_ref):
    tops, sums = top_ref[0 : 4 * CL], sum_ref[0 : 4 * CL]
    top = jnp.max(tops, axis=1, keepdims=True)
    total = jnp.sum(sums * jnp.exp2(tops - top), axis=1)
    return logsum(top[:, 0, :], total)


def pack_kernel(cells_in, extra_in, more_cells_in, more_extra_in, source_in, target_in, out, more_out, codes_out, cells, more_cells, extra, more_extra, source, target, sem):
    copies = [
        pltpu.make_async_copy(a, b, sem.at[k])
        for k, (a, b) in enumerate(
            (
                (cells_in, cells),
                (extra_in, extra),
                (more_cells_in, more_cells),
                (more_extra_in, more_extra),
                (source_in, source),
                (target_in, target),
            )
        )
    ]
    for copy in copies:
        copy.start()
    for k, (a, b, o) in enumerate(((cells, extra, out), (more_cells, more_extra, more_out))):
        copies[2 * k].wait()
        copies[2 * k + 1].wait()
        for n in range(CL):
            o[n, 0:COMP, :] = a[:, n, :]
            o[n, COMP : COMP + 1, :] = b[n : n + 1, :]
            o[n, COMP + 1 : PACKED, :] = jnp.zeros((PACKED - COMP - 1, CELLS), f32)
    copies[4].wait()
    copies[5].wait()
    codes_out[...] = jnp.where(target[...] >= 0, source[...] * CL + target[...], -1)


def row_kernel(codes_in, s0, s1, s2, s3, t0, t1, t2, t3, out, list_out, xn, yn, mass, square_out, codes, list_ref, yt, top, tot, *rest):
    scores, tops, sem = rest[:DEEP], rest[DEEP : 2 * DEEP], rest[2 * DEEP]
    arriving = pltpu.make_async_copy(codes_in, codes, sem.at[0])
    arriving.start()
    one = jnp.ones((1, CELLS), f32)
    ones = (one, one, one)
    middle = centre(s0)
    for k, ref in enumerate((s0, s1, s2, s3)):
        for a in range(CL):
            head, tail, extra, square = load_cluster(ref, a, middle)
            mass[k * CL + a : k * CL + a + 1, :] = extra
            square_out[k * CL + a : k * CL + a + 1, :] = square
            weight = three_parts(-square * SCALE)
            store_operand(xn, k * CL + a, head * (2.0 * SCALE), tail * (2.0 * SCALE), weight, ones)
    top[...] = jnp.full(top.shape, NEGATIVE, f32)
    tot[...] = jnp.zeros(tot.shape, f32)
    arriving.wait()
    owners = target_owners()
    count = jnp.int32(0)
    y = place()[1]
    for k in range(4):
        for d in range(NX):
            for t in range(4):
                code = codes[d * NY + (y + k) % NY, owners[t]]
                source = k * CL + (code >> 2)
                list_ref[count] = source * 256 + t * CL + (code & 3)
                count = count + (code >= 0).astype(jnp.int32)
    for k in range(2 * DEEP):
        list_ref[count + k] = 4 * CL * 256
    list_ref[LIST - 1] = count
    leaving = pltpu.make_async_copy(list_ref, list_out, sem.at[1])
    leaving.start()
    xn[4 * CL] = jnp.zeros((DEPTH, CELLS), bf16)
    for k, ref in enumerate((t0, t1, t2, t3)):
        for a in range(CL):
            head, tail, prior, square = load_cluster(ref, a, middle)
            weight = three_parts((prior - square) * SCALE)
            store_operand(yn, k * CL + a, head, tail, ones, weight)
            yt[k * CL + a] = yn[k * CL + a].T
    over_pairs(count, list_ref, yt, xn, lambda s, t: (t, s, s), top, tot, scores, tops)
    rows = finish(top, tot).reshape(4, CL, CELLS)
    for k in range(4):
        for m in range(MEMBERS):
            out[m, (y + k) % NY] = rows[k]
    leaving.wait()


def column_kernel(list_in, came, mass, square, x_in, yn, kept, given, own, list_ref, xn, xt, four, top, tot, *rest):
    scores, tops, sem = rest[:DEEP], rest[DEEP : 2 * DEEP], rest[2 * DEEP]
    arriving = pltpu.make_async_copy(list_in, list_ref, sem.at[0])
    arriving.start()
    y = place()[1]
    four[...] = merged([came[m] for m in range(MEMBERS)])
    row = lax.broadcasted_iota(jnp.int32, (16, CELLS), 0)
    for k in range(4):
        rows = four[(y + k) % NY]
        if k == 0:
            own[...] = rows
        for a in range(CL):
            n = k * CL + a
            p = EPSILON * mass[n : n + 1, :] - (EPSILON * LN2) * rows[a : a + 1]
            weight = three_parts((p - square[n : n + 1, :]) * SCALE)
            xn[...] = x_in[n]
            end = xn[48:64, :].astype(f32)
            for part in range(3):
                end = jnp.where(row == 2 + part, weight[part], end)
            xn[48:64, :] = end.astype(bf16)
            xt[n] = xn[...].T
    xt[4 * CL] = jnp.zeros((CELLS, DEPTH), bf16)
    top[...] = jnp.full(top.shape, NEGATIVE, f32)
    tot[...] = jnp.zeros(tot.shape, f32)
    arriving.wait()

    def pick(s, t):
        return s, t, jnp.where(s == 4 * CL, 4 * CL, t)

    over_pairs(list_ref[LIST - 1], list_ref, xt, yn, pick, top, tot, scores, tops)
    columns = finish(top, tot)
    for k in range(2):
        kept[k * CL : (k + 1) * CL, :] = columns[2 * k * CL : (2 * k + 1) * CL]
        given[k * CL : (k + 1) * CL, :] = columns[(2 * k + 1) * CL : (2 * k + 2) * CL]


VMEM = pl.BlockSpec(memory_space=pltpu.VMEM)
ANY = pl.BlockSpec(memory_space=pl.ANY)
HBM = pl.BlockSpec(memory_space=pltpu.HBM)


def work(source_coords, target_coords, source_logmass, target_logmass, target_prior, pair_source, pair_target):
    cells = jax.ShapeDtypeStruct((CL, PACKED, CELLS), f32)
    loose = pltpu.VMEM((COMP, CL, CELLS), f32)
    t, s0, codes = pl.pallas_call(
        pack_kernel,
        out_shape=(cells, cells, jax.ShapeDtypeStruct((1, SLOTS), jnp.int32)),
        in_specs=[HBM] * 6,
        out_specs=(VMEM, VMEM, VMEM),
        scratch_shapes=[loose, loose] + [pltpu.VMEM((CL, CELLS), f32)] * 2
        + [pltpu.VMEM((1, SLOTS), jnp.int32)] * 2
        + [pltpu.SemaphoreType.DMA((6,))],
        compiler_params=pltpu.CompilerParams(vmem_limit_bytes=4 * 2**20),
        name="pack",
    )(
        *(
            pltpu.with_memory_space_constraint(value, pltpu.HBM)
            for value in (
                jnp.transpose(target_coords, (1, 0, 2)),
                target_prior,
                jnp.transpose(source_coords, (1, 0, 2)),
                source_logmass,
                pair_source.reshape(1, SLOTS),
                pair_target.reshape(1, SLOTS),
            )
        )
    )
    t2 = fetched(t, lambda x, y, z, c: (x, y, z + FAR[x], c))
    t0 = fetched(t, lambda x, y, z, c: (x, y, z + NEAR[x], c))
    s1, s2, s3 = (from_y(s0, k) for k in (1, 2, 3))
    codes = exchanged(jnp.broadcast_to(codes, (MEMBERS, SLOTS)), PLANES)
    t1, t3 = from_core(t0), from_core(t2)
    shards = (s0, s1, s2, s3, t0, t1, t2, t3)

    shared = (
        [pltpu.VMEM((4 * CL + 1, 8, CELLS), f32)] * 2
        + [pltpu.VMEM((CELLS, CELLS), f32)] * DEEP
        + [pltpu.VMEM((8, CELLS), f32)] * DEEP
        + [pltpu.SemaphoreType.DMA((2,))]
    )
    params = pltpu.CompilerParams(vmem_limit_bytes=16 * 2**20)
    rows, pairs, xn, yn, mass, square = pl.pallas_call(
        row_kernel,
        out_shape=(
            jax.ShapeDtypeStruct((MEMBERS, 4, CL, CELLS), f32),
            jax.ShapeDtypeStruct((LIST,), jnp.int32),
            jax.ShapeDtypeStruct((4 * CL + 1, DEPTH, CELLS), bf16),
            jax.ShapeDtypeStruct((4 * CL, DEPTH, CELLS), bf16),
            jax.ShapeDtypeStruct((4 * CL, CELLS), f32),
            jax.ShapeDtypeStruct((4 * CL, CELLS), f32),
        ),
        in_specs=[ANY] + [VMEM] * 8,
        out_specs=(VMEM, ANY, VMEM, VMEM, VMEM, VMEM),
        scratch_shapes=[
            pltpu.SMEM((MEMBERS, SLOTS), jnp.int32),
            pltpu.SMEM((LIST,), jnp.int32),
            pltpu.VMEM((4 * CL, CELLS, DEPTH), bf16),
        ]
        + shared,
        compiler_params=params,
        name="rows",
    )(codes, *shards)

    rows = exchanged(rows, PLANES)

    kept, given, own = pl.pallas_call(
        column_kernel,
        out_shape=(
            jax.ShapeDtypeStruct((2 * CL, CELLS), f32),
            jax.ShapeDtypeStruct((2 * CL, CELLS), f32),
            jax.ShapeDtypeStruct((CL, CELLS), f32),
        ),
        in_specs=[ANY] + [VMEM] * 5,
        out_specs=(VMEM, VMEM, VMEM),
        scratch_shapes=[
            pltpu.SMEM((LIST,), jnp.int32),
            pltpu.VMEM((DEPTH, CELLS), bf16),
            pltpu.VMEM((4 * CL + 1, CELLS, DEPTH), bf16),
            pltpu.VMEM((4, CL, CELLS), f32),
        ]
        + shared,
        compiler_params=params,
        name="columns",
    )(pairs, rows, mass, square, xn, yn)

    kept = merged([kept, from_core(given)])
    first = fetched(kept[:CL], lambda x, y, z, c: (x, y, z - NEAR[x], c))
    second = fetched(kept[CL:], lambda x, y, z, c: (x, y, z - FAR[x], c))
    part = merged([first, second])
    part = merged([part] + [from_x(part, k) for k in (1, 2, 3)])
    target_potential = EPSILON * target_logmass + target_prior - (EPSILON * LN2) * part
    source_potential = EPSILON * source_logmass - (EPSILON * LN2) * own
    return source_potential, target_potential


def solution(mesh):
    return jax.shard_map(
        work,
        mesh=mesh,
        in_specs=(
            P("own", None, None),
            P("own", None, None),
            P("own", None),
            P("own", None),
            P("own", None),
            P("own", "split", None, None),
            P("own", "split", None, None),
        ),
        out_specs=(P("own", None), P("own", None)),
        check_vma=False,
    )
```
